32 devices in a mesh: blk: 8 (over y, x, core), wide: 4 (over z).
Axes of the slice: x: 2, y: 2, z: 4, core: 2. Of those that a mesh axis runs over, the one named last changes fastest.
Arguments:
- points: bfloat16 [8192, 32], P(('blk', 'wide')), may hold values from -6 to 6
- inv_length: float32 [32], replicated, may hold values from 0.2 to 0.7
- noise_var: float32 [], replicated, may hold values from 0.1 to 1
- solution: float32 [8192, 128], P(('blk', 'wide')), may hold values from -6 to 6
- residual: float32 [8192, 128], P(('blk', 'wide')), may hold values from -6 to 6
- direction: float32 [8192, 128], P(('blk', 'wide')), may hold values from -6 to 6
Outputs:
- new_solution: float32 [8192, 128], P(('blk', 'wide'))
- new_residual: float32 [8192, 128], P(('blk', 'wide'))
- new_direction: float32 [8192, 128], P(('blk', 'wide'))
The draws below stay inside these ranges and needn't reach their ends.
All inputs are finite; a program needn't handle non-finite values.
Results may differ from the reference program's by a relative error of at most 0.01.
Values may be sent and summed in bfloat16 or wider, within the bound.
A program may use at most 64 MiB of HBM per device.

```python
import math
import jax
import jax.numpy as jnp
from jax import lax

PIECE = 256
FEATURES = 32
RHS = 128
POINTS = 8192


def levels(rng, extent, shards, low, largest):
    def one(position, shards_of):
        steps = jax.random.uniform(jax.random.fold_in(jax.random.fold_in(rng, 6), position), (shards_of,), jnp.float32, low / len(shards), largest / len(shards))
        return jnp.repeat(jnp.exp(steps), extent[position] // shards_of).reshape((-1,) + (1,) * (len(extent) - position - 1))

    gain = one(*shards[0])
    for cut in shards[1:]:
        gain = gain * one(*cut)
    return gain


def noise(own_key, extent, spread, limit, cuts=(), kind=jnp.bfloat16):
    gain = levels(own_key, extent, cuts, -0.22, 0.18) if cuts else 1.0
    result = jax.random.normal(own_key, extent, jnp.float32) * spread * gain
    return jnp.minimum(jnp.maximum(result, -limit), limit).astype(kind)


def setup_inputs(seed: int = 0) -> dict:
    seeds = jax.random.split(jax.random.key(seed), 7)
    return {
        "points": noise(seeds[0], (POINTS, FEATURES), 1.0, 6.0, ((0, 32),)),
        "inv_length": jnp.clip(jnp.exp(jax.random.uniform(seeds[1], (FEATURES,), jnp.float32, math.log(0.2), math.log(0.7))), 0.2, 0.7),
        "noise_var": jnp.clip(jnp.exp(jax.random.uniform(seeds[2], (), jnp.float32, math.log(0.1), math.log(1.0))), 0.1, 1.0),
        "solution": noise(seeds[3], (POINTS, RHS), 1.0, 6.0, ((0, 32),), jnp.float32),
        "residual": noise(seeds[4], (POINTS, RHS), 1.0, 6.0, ((0, 32),), jnp.float32),
        "direction": noise(seeds[5], (POINTS, RHS), 1.0, 6.0, ((0, 32),), jnp.float32),
    }


def kernel_tile(rows_x, rows_sq, cols_x, cols_sq):
    inner_prod = jnp.dot(rows_x, cols_x.T, precision=lax.Precision.HIGHEST)
    dist_sq = jnp.maximum(rows_sq[:, None] + cols_sq[None, :] - 2.0 * inner_prod, 0.0)
    radius = jnp.sqrt(5.0 * dist_sq)
    rounded = ((1.0 + radius + radius * radius / 3.0) * jnp.exp(-radius)).astype(jnp.bfloat16)
    return lax.optimization_barrier(rounded).astype(jnp.float32)

def reference(points, inv_length, noise_var, solution, residual, direction):
    scaled = (points.astype(jnp.float32) * inv_length).astype(jnp.bfloat16)
    low_dir = direction.astype(jnp.bfloat16)
    wide_x = lax.optimization_barrier(scaled).astype(jnp.float32)
    wide_p = lax.optimization_barrier(low_dir).astype(jnp.float32)
    point_sq = lax.optimization_barrier(jnp.sum(wide_x * wide_x, axis=1))

    def row_block(block_index):
        start = (block_index * PIECE).astype(jnp.int32)
        rows_x = lax.dynamic_slice_in_dim(wide_x, start, PIECE, 0)
        rows_sq = lax.dynamic_slice_in_dim(point_sq, start, PIECE, 0)
        kernel_rows = kernel_tile(rows_x, rows_sq, wide_x, point_sq)
        return jnp.dot(kernel_rows, wide_p, precision=lax.Precision.HIGHEST)
    blocks = lax.map(row_block, jnp.arange(POINTS // PIECE, dtype=jnp.int32))
    kernel_image = blocks.reshape(POINTS, RHS) + noise_var * direction
    old_norm = lax.optimization_barrier(jnp.sum(residual * residual, axis=0))
    curvature = lax.optimization_barrier(jnp.sum(direction * kernel_image, axis=0))
    step_length = old_norm / curvature
    new_solution = solution + step_length * direction
    new_residual = residual - step_length * kernel_image
    new_norm = lax.optimization_barrier(jnp.sum(new_residual * new_residual, axis=0))
    new_direction = new_residual + new_norm / old_norm * direction
    return (new_solution, new_residual, new_direction)
```

```python
import functools
import math

import jax
import jax.numpy as jnp
from jax import lax
from jax.experimental import pallas as pl
from jax.experimental.pallas import tpu as pltpu
from jax.sharding import PartitionSpec as P

LN2 = math.log(2.0)
SCALE = 5.0 / (LN2 * LN2)
MESH = pl.DeviceIdType.MESH
TAIL = 16


def rounded(x):
    return x.astype(jnp.bfloat16).astype(jnp.float32)


def three_parts(x):
    high = rounded(x)
    rest = x - high
    middle = rounded(rest)
    return high, middle, rounded(rest - middle)


def matern(scaled_dist):
    dist = jnp.maximum(scaled_dist, 1e-30)
    root = dist * lax.rsqrt(dist)
    poly = 1.0 + root * (LN2 + (LN2 * LN2 / 3.0) * root)
    return (poly * jnp.exp2(-root)).astype(jnp.bfloat16)


def kernel(nb, nw, points_in, inv_in, noise_in, residual_in, direction_in, solution_in, solution_out, residual_out, direction_out,
           points, inv_length, noise_var, residual, direction, old_solution, io, feat, feat_z, rows_x, kmat, low_dir, part, part_in, stat, stat_z, stat_b, stat_o,
           fs, fr, fzs, fzr, ps, pr, qs, qr, zs, zr, bs, br):
    b = lax.axis_index("blk")
    w = lax.axis_index("wide")
    chips = nb // 2
    chip, core = b // 2, b % 2
    features, piece = points.shape

    def same_core(q):
        return (lax.rem(chip + q, chips) * 2 + core, w)

    sibling = (chip * 2 + 1 - core, w)

    def along(q):
        return (b, lax.rem(w + q, nw))

    def plane(slot):
        return (lax.rem(chip + slot // 2, chips) * 2 + (core if slot % 2 == 0 else 1 - core), w)

    def back(slot):
        return (chips - slot // 2) % chips * 2 + slot % 2

    barrier = pltpu.get_barrier_semaphore()
    for slot in range(1, nb):
        pl.semaphore_signal(barrier, inc=1, device_id=plane(slot), device_id_type=MESH)
    for q in range(1, nw):
        pl.semaphore_signal(barrier, inc=1, device_id=along(q), device_id_type=MESH)

    def copy(src, dst, send, recv, to):
        return pltpu.make_async_remote_copy(
            src_ref=src, dst_ref=dst, send_sem=send, recv_sem=recv, device_id=to, device_id_type=MESH
        )

    loads = [
        pltpu.make_async_copy(src, dst, io.at[k])
        for k, (src, dst) in enumerate(
            ((points_in, points), (inv_in, inv_length), (direction_in, direction),
             (residual_in, residual), (solution_in, old_solution))
        )
    ]
    for load in loads:
        load.start()
    for load in loads[:2]:
        load.wait()

    inv_row = jnp.concatenate(
        [inv_length[...], jnp.zeros((1, 128 - features), jnp.float32)], axis=1)
    inv_column = jnp.broadcast_to(inv_row, (8, 128)).T[:features, 0:1]
    x_t = rounded(points[...].astype(jnp.float32) * inv_column)
    s1, s2, s3 = three_parts(SCALE * jnp.sum(x_t * x_t, axis=0, keepdims=True))
    row = lax.broadcasted_iota(jnp.int32, (TAIL, piece), 0)
    tail = jnp.where((row >= 3) & (row <= 10), 1.0, 0.0)
    tail = jnp.where((row >= 6) & (row <= 7), 0.0, tail)
    for at, value in ((0, s1), (1, s2), (2, s3), (11, s1), (12, s2), (13, s3)):
        tail = jnp.where(row == at, value, tail)
    feat[0] = jnp.concatenate([x_t, tail], axis=0).astype(jnp.bfloat16)
    for load in loads[2:]:
        load.wait()
    low_dir[0:piece] = direction[...].astype(jnp.bfloat16)
    pl.semaphore_wait(barrier, nb - 1 + nw - 1)

    upper = lax.div(2 * w, nw)

    def near(k):
        return k + upper * (nw - 2 * k)

    def rows_at(q):
        return pl.ds(pl.multiple_of(q * piece, piece), piece)

    sends = []

    def go(c):
        c.start()
        sends.append(c)
        return c

    def feat_copy(src_slot, dst_slot, to):
        return copy(feat.at[src_slot], feat.at[dst_slot], fs.at[dst_slot], fr.at[dst_slot], to)

    def dir_copy(src_slot, dst_slot, to):
        return copy(low_dir.at[pl.ds(src_slot * piece, piece)], low_dir.at[pl.ds(dst_slot * piece, piece)],
                    ps.at[dst_slot], pr.at[dst_slot], to)

    for k in range(1, nw):
        q = near(nw - k)
        go(copy(feat.at[0], feat_z.at[nw - q], fzs.at[q], fzr.at[nw - q], along(q)))
    go(feat_copy(0, 1, sibling))
    for q in range(1, chips):
        go(feat_copy(0, 2 * (chips - q), same_core(q)))
    for q in range(1, chips):
        go(dir_copy(0, 2 * (chips - q), same_core(q)))
    go(dir_copy(0, 1, sibling))

    def feat_arrived(slot):
        feat_copy(slot, slot, sibling).wait_recv()

    def dir_arrived(slot):
        dir_copy(slot, slot, sibling).wait_recv()

    def as_rows(block):
        block = block.astype(jnp.float32)
        x = block[:features]
        h, m, l = three_parts(SCALE * x)
        lanes = jnp.concatenate(
            [-2.0 * h, -2.0 * m, -2.0 * l, block[features + 8 :],
             jnp.zeros((TAIL + 8, piece), jnp.float32)], axis=0)
        return lanes.T.astype(jnp.bfloat16)

    depth = rows_x.shape[1]

    def tile(at, slot):
        block = feat[slot]
        cols = jnp.concatenate(
            [block[:features]] * 3 + [block[features:],
             jnp.zeros((depth - 3 * features - TAIL, piece), jnp.bfloat16)], axis=0)
        dist = jnp.dot(rows_x[at, :], cols, preferred_element_type=jnp.float32)
        kmat[at, slot * piece : (slot + 1) * piece] = matern(dist)

    def feat_z_arrived(q):
        copy(feat_z.at[q], feat_z.at[q], fzs.at[q], fzr.at[q], along(q)).wait_recv()

    def relay_direction(q):
        dir_arrived(2 * q)
        go(dir_copy(2 * q, 2 * q + 1, sibling))

    rows_x[0:piece] = as_rows(feat[0])
    tile(pl.ds(0, piece), 0)
    feat_arrived(1)
    tile(pl.ds(0, piece), 1)
    for q in range(1, chips):
        feat_arrived(2 * q)
        go(feat_copy(2 * q, 2 * q + 1, sibling))
        tile(pl.ds(0, piece), 2 * q)
    for q in range(1, chips):
        feat_arrived(2 * q + 1)
        tile(pl.ds(0, piece), 2 * q + 1)
    if nw <= 4:
        relayed = 1
        for k in range(1, nw):
            q = near(k)
            feat_z_arrived(q)
            rows_x[rows_at(q), :] = as_rows(feat_z[q])
            for slot in range(nb):
                tile(rows_at(q), slot)
                if k == nw - 1 and slot in (0, nb // 2) and relayed < chips:
                    relay_direction(relayed)
                    relayed += 1
    else:
        relayed = 1
        for q in range(1, nw):
            feat_z_arrived(q)
            rows_x[q * piece : (q + 1) * piece] = as_rows(feat_z[q])

        def row_tiles(q, carry):
            for slot in range(nb):
                tile(pl.ds(pl.multiple_of(q * piece, piece), piece), slot)
            return carry

        lax.fori_loop(1, nw, row_tiles, 0)
    for q in range(relayed, chips):
        relay_direction(q)
    for q in range(chips):
        dir_arrived(2 * q + 1)

    def partial(q):
        return jnp.dot(kmat[rows_at(q), :], low_dir[...],
                       preferred_element_type=jnp.float32)

    for k in range(1, nw):
        q = near(nw - k)
        part[q] = partial(q).astype(jnp.bfloat16)
        go(copy(part.at[q], part_in.at[nw - q], qs.at[q], qr.at[nw - q], along(q)))
    total = partial(0) + noise_in[0, 0] * direction[...]
    for q in range(1, nw):
        copy(part.at[q], part_in.at[q], qs.at[q], qr.at[q], along(q)).wait_recv()
        total = total + part_in[q].astype(jnp.float32)

    def column_sum(x):
        return jnp.sum(x, axis=0, keepdims=True)

    res, direc = residual[...], direction[...]
    at = lax.broadcasted_iota(jnp.int32, (8, res.shape[1]), 0)
    sums = jnp.zeros(at.shape, jnp.float32)
    for k, value in enumerate((res * res, direc * total, res * total, total * total)):
        sums = jnp.where(at == k, column_sum(value), sums)
    stat[...] = sums
    for q in range(1, nw):
        go(copy(stat, stat_z.at[nw - q], zs.at[q], zr.at[nw - q], along(q)))
    for q in range(1, nw):
        copy(stat, stat_z.at[q], zs.at[q], zr.at[q], along(q)).wait_recv()
        sums = sums + stat_z[q]
    stat_o[...] = sums
    for slot in range(1, nb):
        go(copy(stat_o, stat_b.at[back(slot)], bs.at[slot], br.at[back(slot)], plane(slot)))
    for slot in range(1, nb):
        copy(stat_o, stat_b.at[slot], bs.at[slot], br.at[slot], plane(slot)).wait_recv()
        sums = sums + stat_b[slot]
    old_norm, step = sums[0:1], sums[0:1] / sums[1:2]
    new_norm = old_norm - 2.0 * step * sums[2:3] + step * step * sums[3:4]
    new_residual = res - step * total
    residual_out[...] = new_residual
    solution_out[...] = old_solution[...] + step * direc
    direction_out[...] = new_residual + new_norm / old_norm * direc
    for c in sends:
        c.wait_send()


def write_out(a, b, c, a_out, b_out, c_out, sems):
    copies = [
        pltpu.make_async_copy(src, dst, sems.at[k])
        for k, (src, dst) in enumerate(((a, a_out), (b, b_out), (c, c_out)))
    ]
    for copy in copies:
        copy.start()
    for copy in copies:
        copy.wait()


def on_device(nb, nw, points, inv_length, noise_var, solution, residual, direction):
    piece, features = points.shape
    rhs = direction.shape[1]
    vmem = pl.BlockSpec(memory_space=pltpu.VMEM)
    hbm = pl.BlockSpec(memory_space=pl.ANY)
    dma = pltpu.SemaphoreType.DMA
    depth = 3 * features + 2 * TAIL
    news = pl.pallas_call(
        functools.partial(kernel, nb, nw),
        out_shape=(pltpu.VMEM((piece, rhs), jnp.float32),) * 3,
        in_specs=[hbm, hbm, pl.BlockSpec(memory_space=pltpu.SMEM), hbm, hbm, hbm],
        out_specs=(vmem,) * 3,
        scratch_shapes=[
            pltpu.VMEM((features, piece), points.dtype),
            pltpu.VMEM((1, features), jnp.float32),
            pltpu.VMEM((1, 1), jnp.float32),
            pltpu.VMEM((piece, rhs), jnp.float32),
            pltpu.VMEM((piece, rhs), jnp.float32),
            pltpu.VMEM((piece, rhs), jnp.float32),
            dma((6,)),
            pltpu.VMEM((nb, features + TAIL, piece), jnp.bfloat16),
            pltpu.VMEM((nw, features + TAIL, piece), jnp.bfloat16),
            pltpu.VMEM((nw * piece, depth), jnp.bfloat16),
            pltpu.VMEM((nw * piece, nb * piece), jnp.bfloat16),
            pltpu.VMEM((nb * piece, rhs), jnp.bfloat16),
            pltpu.VMEM((nw, piece, rhs), jnp.bfloat16),
            pltpu.VMEM((nw, piece, rhs), jnp.bfloat16),
            pltpu.VMEM((8, rhs), jnp.float32),
            pltpu.VMEM((nw, 8, rhs), jnp.float32),
            pltpu.VMEM((nb, 8, rhs), jnp.float32),
            pltpu.VMEM((8, rhs), jnp.float32),
            dma((nb,)), dma((nb,)), dma((nw,)), dma((nw,)), dma((nb,)), dma((nb,)),
            dma((nw,)), dma((nw,)), dma((nw,)), dma((nw,)), dma((nb,)), dma((nb,)),
        ],
        compiler_params=pltpu.CompilerParams(
            collective_id=0, has_side_effects=True, vmem_limit_bytes=60 * 1024 * 1024
        ),
    )(points.T, inv_length.reshape(1, features), noise_var.reshape(1, 1), residual, direction, solution)
    return pl.pallas_call(
        write_out,
        out_shape=(jax.ShapeDtypeStruct((piece, rhs), jnp.float32),) * 3,
        in_specs=[vmem] * 3,
        out_specs=(hbm,) * 3,
        scratch_shapes=[dma((3,))],
    )(*(pltpu.with_memory_space_constraint(x, pltpu.VMEM) for x in news))


def solution(mesh):
    spec = P(("blk", "wide"), None)
    return jax.shard_map(
        functools.partial(on_device, mesh.shape["blk"], mesh.shape["wide"]),
        mesh=mesh,
        in_specs=(spec, P(), P(), spec, spec, spec),
        out_specs=(spec, spec, spec),
        check_vma=False,
    )
```

```python
import functools
import math

import jax
import jax.numpy as jnp
from jax import lax
from jax.experimental import pallas as pl
from jax.experimental.pallas import tpu as pltpu
from jax.sharding import PartitionSpec as P

LN2 = math.log(2.0)
SCALE = 5.0 / (LN2 * LN2)
MESH = pl.DeviceIdType.MESH
TAIL = 16


def rounded(x):
    return x.astype(jnp.bfloat16).astype(jnp.float32)


def three_parts(x):
    high = rounded(x)
    rest = x - high
    middle = rounded(rest)
    return high, middle, rounded(rest - middle)


def matern(scaled_dist):
    dist = jnp.maximum(scaled_dist, 1e-30)
    root = dist * lax.rsqrt(dist)
    poly = 1.0 + root * (LN2 + (LN2 * LN2 / 3.0) * root)
    return (poly * jnp.exp2(-root)).astype(jnp.bfloat16)


def kernel(nb, nw, points_in, inv_in, noise_in, residual_in, direction_in, solution_in, solution_out, residual_out, direction_out,
           points, inv_length, residual, direction, old_solution, io, feat, feat_z, rows_x, kmat, low_dir, acc, part, part_in, stat, stat_in,
           fs, fr, fzs, fzr, ps, pr, qs, qr, ss, sr):
    b = lax.axis_index("blk")
    w = lax.axis_index("wide")
    chips = nb // 2
    chip, core = b // 2, b % 2
    features, piece = points.shape

    def other_chip(k):
        at, bit = chip, 1
        while bit < chips:
            if k & bit:
                at = at + bit - 2 * bit * lax.rem(lax.div(chip, bit), 2)
            bit *= 2
        return at

    def same_core(k):
        return (other_chip(k) * 2 + core, w)

    sibling = (chip * 2 + 1 - core, w)

    def along(q):
        return (b, lax.rem(w + q, nw))

    def at_least(limit):
        return lax.div(w + nw - limit, nw)

    upper = lax.div(2 * w, nw)

    def far_first(k):
        low = nw - 1 - k - at_least(nw - 1 - k)
        high = k + 1 - at_least(k + 1)
        return lax.rem(low + upper * (high - low) - w + nw, nw)

    z_far = [far_first(k) for k in range(nw - 1)]
    chips_far = sorted(range(1, chips), key=lambda k: -bin(k).count("1"))
    chips_near = chips_far[::-1]

    barrier = pltpu.get_barrier_semaphore()
    for k in range(1, chips):
        pl.semaphore_signal(barrier, inc=1, device_id=same_core(k), device_id_type=MESH)
    pl.semaphore_signal(barrier, inc=1, device_id=sibling, device_id_type=MESH)
    for q in range(1, nw):
        pl.semaphore_signal(barrier, inc=1, device_id=along(q), device_id_type=MESH)

    def copy(src, dst, send, recv, to):
        return pltpu.make_async_remote_copy(
            src_ref=src, dst_ref=dst, send_sem=send, recv_sem=recv, device_id=to, device_id_type=MESH
        )

    loads = [
        pltpu.make_async_copy(src, dst, io.at[k])
        for k, (src, dst) in enumerate(
            ((points_in, points), (inv_in, inv_length), (direction_in, direction),
             (residual_in, residual), (solution_in, old_solution))
        )
    ]
    for load in loads:
        load.start()
    for load in loads[:2]:
        load.wait()

    inv_row = jnp.concatenate(
        [inv_length[...], jnp.zeros((1, 128 - features), jnp.float32)], axis=1)
    inv_column = jnp.broadcast_to(inv_row, (8, 128)).T[:features, 0:1]
    x_t = rounded(points[...].astype(jnp.float32) * inv_column)
    s1, s2, s3 = three_parts(SCALE * jnp.sum(x_t * x_t, axis=0, keepdims=True))
    row = lax.broadcasted_iota(jnp.int32, (TAIL, piece), 0)
    tail = jnp.where((row >= 3) & (row <= 10), 1.0, 0.0)
    tail = jnp.where((row >= 6) & (row <= 7), 0.0, tail)
    for at, value in ((0, s1), (1, s2), (2, s3), (11, s1), (12, s2), (13, s3)):
        tail = jnp.where(row == at, value, tail)
    feat[0] = jnp.concatenate([x_t, tail], axis=0).astype(jnp.bfloat16)
    loads[2].wait()
    low_dir[0:piece] = direction[...].astype(jnp.bfloat16)
    pl.semaphore_wait(barrier, chips + nw - 1)

    sends = []

    def go(c):
        c.start()
        sends.append(c)
        return c

    def feat_copy(src_slot, dst_slot, to):
        return copy(feat.at[src_slot], feat.at[dst_slot], fs.at[dst_slot], fr.at[dst_slot], to)

    def dir_copy(src_slot, dst_slot, to):
        return copy(low_dir.at[pl.ds(src_slot * piece, piece)], low_dir.at[pl.ds(dst_slot * piece, piece)],
                    ps.at[dst_slot], pr.at[dst_slot], to)

    for q in z_far:
        go(copy(feat.at[0], feat_z.at[nw - q], fzs.at[q], fzr.at[nw - q], along(q)))
    for k in chips_far:
        go(feat_copy(0, k, same_core(k)))
    go(feat_copy(0, chips, sibling))
    for k in chips_far:
        go(dir_copy(0, k, same_core(k)))
    go(dir_copy(0, chips, sibling))
    for load in loads[3:]:
        load.wait()

    def feat_arrived(slot):
        feat_copy(slot, slot, sibling).wait_recv()

    def dir_arrived(slot):
        dir_copy(slot, slot, sibling).wait_recv()

    def relay_feat(k):
        feat_arrived(k)
        go(feat_copy(k, chips + k, sibling))

    def relay_dir(k):
        dir_arrived(k)
        go(dir_copy(k, chips + k, sibling))

    def as_rows(block):
        block = block.astype(jnp.float32)
        x = block[:features]
        h, m, l = three_parts(SCALE * x)
        lanes = jnp.concatenate(
            [-2.0 * h, -2.0 * m, -2.0 * l, block[features + 8 :],
             jnp.zeros((TAIL + 8, piece), jnp.float32)], axis=0)
        return lanes.T.astype(jnp.bfloat16)

    depth = rows_x.shape[1]

    def tiles(rows, slot):
        block = feat[slot]
        cols = jnp.concatenate(
            [block[:features]] * 3 + [block[features:],
             jnp.zeros((depth - 3 * features - TAIL, piece), jnp.bfloat16)], axis=0)
        for j in rows:
            dist = jnp.dot(rows_x[j * piece : (j + 1) * piece, :], cols, preferred_element_type=jnp.float32)
            kmat[j * piece : (j + 1) * piece, slot * piece : (slot + 1) * piece] = matern(dist)

    rows_x[0:piece] = as_rows(feat[0])
    tiles([0], 0)
    feat_arrived(chips)
    tiles([0], chips)
    for j in range(1, nw):
        q = z_far[nw - 1 - j]
        copy(feat_z.at[q], feat_z.at[q], fzs.at[q], fzr.at[q], along(q)).wait_recv()
        rows_x[j * piece : (j + 1) * piece] = as_rows(feat_z[q])
        tiles([j], 0)
        tiles([j], chips)
    every = range(nw)
    for at, k in enumerate(chips_near):
        relay_feat(k)
        if at:
            tiles(every, chips_near[at - 1])
    tiles(every, chips_near[-1])
    for k in chips_near:
        feat_arrived(chips + k)
        tiles(every, chips + k)
        relay_dir(k)

    half = chips * piece

    def product(j, side):
        return jnp.dot(kmat[j * piece : (j + 1) * piece, side * half : (side + 1) * half],
                       low_dir[side * half : (side + 1) * half], preferred_element_type=jnp.float32)

    for j in every:
        acc[j] = product(j, 0)
    for k in range(chips):
        dir_arrived(chips + k)
    for k in range(nw - 1):
        j, q = nw - 1 - k, z_far[k]
        part[j] = (acc[j] + product(j, 1)).astype(jnp.bfloat16)
        go(copy(part.at[j], part_in.at[nw - q], qs.at[j], qr.at[nw - q], along(q)))
    res, direc = residual[...], direction[...]
    total = acc[0] + product(0, 1) + noise_in[0, 0] * direc
    for q in range(1, nw):
        copy(part_in.at[q], part_in.at[q], qs.at[q], qr.at[q], along(q)).wait_recv()
        total = total + part_in[q].astype(jnp.float32)

    for k, value in enumerate((res * res, direc * total, res * total, total * total)):
        stat[k : k + 1] = jnp.sum(value, axis=0, keepdims=True)
    for r, q in enumerate(z_far + [0]):
        for k in chips_far + [0]:
            for c in range(2):
                if r == nw - 1 and k == 0 and c == 0:
                    continue
                to = (other_chip(k) * 2 + (core if c == 0 else 1 - core), lax.rem(w + q, nw))
                slot = (lax.rem(nw - q, nw) * 2 + c) * chips + k
                go(copy(stat, stat_in.at[slot], ss.at[0], sr.at[0], to))
    others = stat_in.at[pl.ds(1, nb * nw - 1)]
    copy(others, others, ss.at[0], sr.at[0], sibling).wait_recv()
    sums = stat[...]
    for slot in range(1, nb * nw):
        sums = sums + stat_in[slot]
    old_norm, step = sums[0:1], sums[0:1] / sums[1:2]
    new_norm = old_norm - 2.0 * step * sums[2:3] + step * step * sums[3:4]
    new_residual = res - step * total
    residual_out[...] = new_residual
    solution_out[...] = old_solution[...] + step * direc
    direction_out[...] = new_residual + new_norm / old_norm * direc
    for c in sends[: len(sends) - (nb * nw - 1)]:
        c.wait_send()
    copy(others, others, ss.at[0], sr.at[0], sibling).wait_send()


def long_kernel(nb, nw, points_in, inv_in, noise_in, residual_in, direction_in, solution_in, solution_out, residual_out, direction_out,
           points, inv_length, noise_var, residual, direction, old_solution, io, feat, feat_z, rows_x, kmat, low_dir, part, part_in, stat, stat_z, stat_b, stat_o,
           fs, fr, fzs, fzr, ps, pr, qs, qr, zs, zr, bs, br):
    b = lax.axis_index("blk")
    w = lax.axis_index("wide")
    chips = nb // 2
    chip, core = b // 2, b % 2
    features, piece = points.shape

    def same_core(q):
        return (lax.rem(chip + q, chips) * 2 + core, w)

    sibling = (chip * 2 + 1 - core, w)

    def along(q):
        return (b, lax.rem(w + q, nw))

    def plane(slot):
        return (lax.rem(chip + slot // 2, chips) * 2 + (core if slot % 2 == 0 else 1 - core), w)

    def back(slot):
        return (chips - slot // 2) % chips * 2 + slot % 2

    barrier = pltpu.get_barrier_semaphore()
    for slot in range(1, nb):
        pl.semaphore_signal(barrier, inc=1, device_id=plane(slot), device_id_type=MESH)
    for q in range(1, nw):
        pl.semaphore_signal(barrier, inc=1, device_id=along(q), device_id_type=MESH)

    def copy(src, dst, send, recv, to):
        return pltpu.make_async_remote_copy(
            src_ref=src, dst_ref=dst, send_sem=send, recv_sem=recv, device_id=to, device_id_type=MESH
        )

    loads = [
        pltpu.make_async_copy(src, dst, io.at[k])
        for k, (src, dst) in enumerate(
            ((points_in, points), (inv_in, inv_length), (direction_in, direction),
             (residual_in, residual), (solution_in, old_solution))
        )
    ]
    for load in loads:
        load.start()
    for load in loads[:2]:
        load.wait()

    inv_row = jnp.concatenate(
        [inv_length[...], jnp.zeros((1, 128 - features), jnp.float32)], axis=1)
    inv_column = jnp.broadcast_to(inv_row, (8, 128)).T[:features, 0:1]
    x_t = rounded(points[...].astype(jnp.float32) * inv_column)
    s1, s2, s3 = three_parts(SCALE * jnp.sum(x_t * x_t, axis=0, keepdims=True))
    row = lax.broadcasted_iota(jnp.int32, (TAIL, piece), 0)
    tail = jnp.where((row >= 3) & (row <= 10), 1.0, 0.0)
    tail = jnp.where((row >= 6) & (row <= 7), 0.0, tail)
    for at, value in ((0, s1), (1, s2), (2, s3), (11, s1), (12, s2), (13, s3)):
        tail = jnp.where(row == at, value, tail)
    feat[0] = jnp.concatenate([x_t, tail], axis=0).astype(jnp.bfloat16)
    for load in loads[2:]:
        load.wait()
    low_dir[0:piece] = direction[...].astype(jnp.bfloat16)
    pl.semaphore_wait(barrier, nb - 1 + nw - 1)

    upper = lax.div(2 * w, nw)

    def near(k):
        return k + upper * (nw - 2 * k)

    def rows_at(q):
        return pl.ds(pl.multiple_of(q * piece, piece), piece)

    sends = []

    def go(c):
        c.start()
        sends.append(c)
        return c

    def feat_copy(src_slot, dst_slot, to):
        return copy(feat.at[src_slot], feat.at[dst_slot], fs.at[dst_slot], fr.at[dst_slot], to)

    def dir_copy(src_slot, dst_slot, to):
        return copy(low_dir.at[pl.ds(src_slot * piece, piece)], low_dir.at[pl.ds(dst_slot * piece, piece)],
                    ps.at[dst_slot], pr.at[dst_slot], to)

    for k in range(1, nw):
        q = near(nw - k)
        go(copy(feat.at[0], feat_z.at[nw - q], fzs.at[q], fzr.at[nw - q], along(q)))
    go(feat_copy(0, 1, sibling))
    for q in range(1, chips):
        go(feat_copy(0, 2 * (chips - q), same_core(q)))
    for q in range(1, chips):
        go(dir_copy(0, 2 * (chips - q), same_core(q)))
    go(dir_copy(0, 1, sibling))

    def feat_arrived(slot):
        feat_copy(slot, slot, sibling).wait_recv()

    def dir_arrived(slot):
        dir_copy(slot, slot, sibling).wait_recv()

    def as_rows(block):
        block = block.astype(jnp.float32)
        x = block[:features]
        h, m, l = three_parts(SCALE * x)
        lanes = jnp.concatenate(
            [-2.0 * h, -2.0 * m, -2.0 * l, block[features + 8 :],
             jnp.zeros((TAIL + 8, piece), jnp.float32)], axis=0)
        return lanes.T.astype(jnp.bfloat16)

    depth = rows_x.shape[1]

    def tile(at, slot):
        block = feat[slot]
        cols = jnp.concatenate(
            [block[:features]] * 3 + [block[features:],
             jnp.zeros((depth - 3 * features - TAIL, piece), jnp.bfloat16)], axis=0)
        dist = jnp.dot(rows_x[at, :], cols, preferred_element_type=jnp.float32)
        kmat[at, slot * piece : (slot + 1) * piece] = matern(dist)

    def feat_z_arrived(q):
        copy(feat_z.at[q], feat_z.at[q], fzs.at[q], fzr.at[q], along(q)).wait_recv()

    def relay_direction(q):
        dir_arrived(2 * q)
        go(dir_copy(2 * q, 2 * q + 1, sibling))

    rows_x[0:piece] = as_rows(feat[0])
    tile(pl.ds(0, piece), 0)
    feat_arrived(1)
    tile(pl.ds(0, piece), 1)
    for q in range(1, chips):
        feat_arrived(2 * q)
        go(feat_copy(2 * q, 2 * q + 1, sibling))
        tile(pl.ds(0, piece), 2 * q)
    for q in range(1, chips):
        feat_arrived(2 * q + 1)
        tile(pl.ds(0, piece), 2 * q + 1)
    if nw <= 4:
        relayed = 1
        for k in range(1, nw):
            q = near(k)
            feat_z_arrived(q)
            rows_x[rows_at(q), :] = as_rows(feat_z[q])
            for slot in range(nb):
                tile(rows_at(q), slot)
                if k == nw - 1 and slot in (0, nb // 2) and relayed < chips:
                    relay_direction(relayed)
                    relayed += 1
    else:
        relayed = 1
        for q in range(1, nw):
            feat_z_arrived(q)
            rows_x[q * piece : (q + 1) * piece] = as_rows(feat_z[q])

        def row_tiles(q, carry):
            for slot in range(nb):
                tile(pl.ds(pl.multiple_of(q * piece, piece), piece), slot)
            return carry

        lax.fori_loop(1, nw, row_tiles, 0)
    for q in range(relayed, chips):
        relay_direction(q)
    for q in range(chips):
        dir_arrived(2 * q + 1)

    def partial(q):
        return jnp.dot(kmat[rows_at(q), :], low_dir[...],
                       preferred_element_type=jnp.float32)

    for k in range(1, nw):
        q = near(nw - k)
        part[q] = partial(q).astype(jnp.bfloat16)
        go(copy(part.at[q], part_in.at[nw - q], qs.at[q], qr.at[nw - q], along(q)))
    total = partial(0) + noise_in[0, 0] * direction[...]
    for q in range(1, nw):
        copy(part.at[q], part_in.at[q], qs.at[q], qr.at[q], along(q)).wait_recv()
        total = total + part_in[q].astype(jnp.float32)

    def column_sum(x):
        return jnp.sum(x, axis=0, keepdims=True)

    res, direc = residual[...], direction[...]
    at = lax.broadcasted_iota(jnp.int32, (8, res.shape[1]), 0)
    sums = jnp.zeros(at.shape, jnp.float32)
    for k, value in enumerate((res * res, direc * total, res * total, total * total)):
        sums = jnp.where(at == k, column_sum(value), sums)
    stat[...] = sums
    for q in range(1, nw):
        go(copy(stat, stat_z.at[nw - q], zs.at[q], zr.at[nw - q], along(q)))
    for q in range(1, nw):
        copy(stat, stat_z.at[q], zs.at[q], zr.at[q], along(q)).wait_recv()
        sums = sums + stat_z[q]
    stat_o[...] = sums
    for slot in range(1, nb):
        go(copy(stat_o, stat_b.at[back(slot)], bs.at[slot], br.at[back(slot)], plane(slot)))
    for slot in range(1, nb):
        copy(stat_o, stat_b.at[slot], bs.at[slot], br.at[slot], plane(slot)).wait_recv()
        sums = sums + stat_b[slot]
    old_norm, step = sums[0:1], sums[0:1] / sums[1:2]
    new_norm = old_norm - 2.0 * step * sums[2:3] + step * step * sums[3:4]
    new_residual = res - step * total
    residual_out[...] = new_residual
    solution_out[...] = old_solution[...] + step * direc
    direction_out[...] = new_residual + new_norm / old_norm * direc
    for c in sends:
        c.wait_send()


def write_out(a, b, c, a_out, b_out, c_out, sems):
    copies = [
        pltpu.make_async_copy(src, dst, sems.at[k])
        for k, (src, dst) in enumerate(((a, a_out), (b, b_out), (c, c_out)))
    ]
    for copy in copies:
        copy.start()
    for copy in copies:
        copy.wait()


def on_device(nb, nw, points, inv_length, noise_var, solution, residual, direction):
    piece, features = points.shape
    rhs = direction.shape[1]
    vmem = pl.BlockSpec(memory_space=pltpu.VMEM)
    hbm = pl.BlockSpec(memory_space=pl.ANY)
    dma = pltpu.SemaphoreType.DMA
    depth = 3 * features + 2 * TAIL
    common = [
        pltpu.VMEM((features, piece), points.dtype),
        pltpu.VMEM((1, features), jnp.float32),
    ]
    wide = [
        dma((6,)),
        pltpu.VMEM((nb, features + TAIL, piece), jnp.bfloat16),
        pltpu.VMEM((nw, features + TAIL, piece), jnp.bfloat16),
        pltpu.VMEM((nw * piece, depth), jnp.bfloat16),
        pltpu.VMEM((nw * piece, nb * piece), jnp.bfloat16),
        pltpu.VMEM((nb * piece, rhs), jnp.bfloat16),
    ]
    vectors = [pltpu.VMEM((piece, rhs), jnp.float32)] * 3
    parts = [pltpu.VMEM((nw, piece, rhs), jnp.bfloat16)] * 2
    sems = [dma((nb,)), dma((nb,)), dma((nw,)), dma((nw,)), dma((nb,)), dma((nb,)), dma((nw,)), dma((nw,))]
    if nw <= 4:
        body = kernel
        scratch = common + vectors + wide + [pltpu.VMEM((nw, piece, rhs), jnp.float32)] + parts + [
            pltpu.VMEM((4, rhs), jnp.float32), pltpu.VMEM((nw * nb, 4, rhs), jnp.float32),
        ] + sems + [dma((1,)), dma((1,))]
    else:
        body = long_kernel
        scratch = common + [pltpu.VMEM((1, 1), jnp.float32)] + vectors + wide + parts + [
            pltpu.VMEM((8, rhs), jnp.float32),
            pltpu.VMEM((nw, 8, rhs), jnp.float32),
            pltpu.VMEM((nb, 8, rhs), jnp.float32),
            pltpu.VMEM((8, rhs), jnp.float32),
        ] + sems + [dma((nw,)), dma((nw,)), dma((nb,)), dma((nb,))]
    news = pl.pallas_call(
        functools.partial(body, nb, nw),
        out_shape=(pltpu.VMEM((piece, rhs), jnp.float32),) * 3,
        in_specs=[hbm, hbm, pl.BlockSpec(memory_space=pltpu.SMEM), hbm, hbm, hbm],
        out_specs=(vmem,) * 3,
        scratch_shapes=scratch,
        compiler_params=pltpu.CompilerParams(
            collective_id=0, has_side_effects=True, vmem_limit_bytes=60 * 1024 * 1024
        ),
    )(points.T, inv_length.reshape(1, features), noise_var.reshape(1, 1), residual, direction, solution)
    return pl.pallas_call(
        write_out,
        out_shape=(jax.ShapeDtypeStruct((piece, rhs), jnp.float32),) * 3,
        in_specs=[vmem] * 3,
        out_specs=(hbm,) * 3,
        scratch_shapes=[dma((3,))],
    )(*(pltpu.with_memory_space_constraint(x, pltpu.VMEM) for x in news))


def solution(mesh):
    spec = P(("blk", "wide"), None)
    return jax.shard_map(
        functools.partial(on_device, mesh.shape["blk"], mesh.shape["wide"]),
        mesh=mesh,
        in_specs=(spec, P(), P(), spec, spec, spec),
        out_specs=(spec, spec, spec),
        check_vma=False,
    )
```

```python
import functools
import math

import jax
import jax.numpy as jnp
from jax import lax
from jax.experimental import pallas as pl
from jax.experimental.pallas import tpu as pltpu
from jax.sharding import PartitionSpec as P

LN2 = math.log(2.0)
SCALE = 5.0 / (LN2 * LN2)
MESH = pl.DeviceIdType.MESH
TAIL = 16


def rounded(x):
    return x.astype(jnp.bfloat16).astype(jnp.float32)


def three_parts(x):
    high = rounded(x)
    rest = x - high
    middle = rounded(rest)
    return high, middle, rounded(rest - middle)


def matern(scaled_dist):
    dist = jnp.maximum(scaled_dist, 1e-30)
    root = dist * lax.rsqrt(dist)
    poly = 1.0 + root * (LN2 + (LN2 * LN2 / 3.0) * root)
    return (poly * jnp.exp2(-root)).astype(jnp.bfloat16)


def kernel(nb, nw, points_in, inv_in, noise_in, residual_in, direction_in, solution_in, solution_out, residual_out, direction_out,
           points, inv_length, residual, direction, old_solution, io, feat, feat_z, rows_x, cols_x, kmat, dir_a, dir_b, part_a, part_a_in, part_b, part_b_in, stat, stat_in,
           fs, fr, fzs, fzr, as_, ar, bs, br, qs, qr, ts, tr, ss, sr):
    b = lax.axis_index("blk")
    w = lax.axis_index("wide")
    chips = nb // 2
    chip, core = b // 2, b % 2
    features, piece = points.shape

    def other_chip(k):
        at, bit = chip, 1
        while bit < chips:
            if k & bit:
                at = at + bit - 2 * bit * lax.rem(lax.div(chip, bit), 2)
            bit *= 2
        return at

    def same_core(k):
        return (other_chip(k) * 2 + core, w)

    sibling = (chip * 2 + 1 - core, w)

    def along(q):
        return (b, lax.rem(w + q, nw))

    def at_least(limit):
        return lax.div(w + nw - limit, nw)

    upper = lax.div(2 * w, nw)

    def far_first(k):
        low = nw - 1 - k - at_least(nw - 1 - k)
        high = k + 1 - at_least(k + 1)
        return lax.rem(low + upper * (high - low) - w + nw, nw)

    z_far = [far_first(k) for k in range(nw - 1)]
    chips_far = sorted(range(1, chips), key=lambda k: -bin(k).count("1"))
    chips_near = chips_far[::-1]

    barrier = pltpu.get_barrier_semaphore()
    for k in range(1, chips):
        pl.semaphore_signal(barrier, inc=1, device_id=same_core(k), device_id_type=MESH)
    pl.semaphore_signal(barrier, inc=1, device_id=sibling, device_id_type=MESH)
    for q in range(1, nw):
        pl.semaphore_signal(barrier, inc=1, device_id=along(q), device_id_type=MESH)

    def copy(src, dst, send, recv, to):
        return pltpu.make_async_remote_copy(
            src_ref=src, dst_ref=dst, send_sem=send, recv_sem=recv, device_id=to, device_id_type=MESH
        )

    loads = [
        pltpu.make_async_copy(src, dst, io.at[k])
        for k, (src, dst) in enumerate(
            ((points_in, points), (inv_in, inv_length), (direction_in, direction),
             (residual_in, residual), (solution_in, old_solution))
        )
    ]
    for load in loads:
        load.start()
    for load in loads[:2]:
        load.wait()

    inv_row = jnp.concatenate(
        [inv_length[...], jnp.zeros((1, 128 - features), jnp.float32)], axis=1)
    inv_column = jnp.broadcast_to(inv_row, (8, 128)).T[:features, 0:1]
    x_t = rounded(points[...].astype(jnp.float32) * inv_column)
    feat[0] = x_t.astype(jnp.bfloat16)
    loads[2].wait()
    dir_t = direction[...].T.astype(jnp.bfloat16)
    part = dir_t.shape[0] // 2
    dir_a[0] = dir_t[:part]
    dir_b[0] = dir_t[part:]
    pl.semaphore_wait(barrier, chips + nw - 1)

    sends = []

    def go(c):
        c.start()
        sends.append(c)
        return c

    def feat_copy(src_slot, dst_slot, to):
        return copy(feat.at[src_slot], feat.at[dst_slot], fs.at[dst_slot], fr.at[dst_slot], to)

    def dir_copy(src_slot, dst_slot, to):
        return copy(dir_a.at[src_slot], dir_a.at[dst_slot], as_.at[dst_slot], ar.at[dst_slot], to)

    for q in z_far:
        go(copy(feat.at[0], feat_z.at[nw - q], fzs.at[q], fzr.at[nw - q], along(q)))
    for k in chips_far:
        go(feat_copy(0, k, same_core(k)))
    go(feat_copy(0, chips, sibling))
    for k in chips_far:
        go(dir_copy(0, k, same_core(k)))
    for q in z_far:
        go(copy(dir_b.at[0], dir_b.at[nw - q], bs.at[q], br.at[nw - q], along(q)))
    go(dir_copy(0, chips, sibling))
    for load in loads[3:]:
        load.wait()

    def feat_arrived(slot):
        feat_copy(slot, slot, sibling).wait_recv()

    def dir_arrived(slot):
        dir_copy(slot, slot, sibling).wait_recv()

    def relay_feat(k):
        feat_arrived(k)
        go(feat_copy(k, chips + k, sibling))

    def relay_dir(k):
        dir_arrived(k)
        go(dir_copy(k, chips + k, sibling))

    depth = rows_x.shape[1]
    ones = jnp.where(lax.broadcasted_iota(jnp.int32, (8, piece), 0) < 3, 1.0, 0.0)
    at = lax.broadcasted_iota(jnp.int32, (8, piece), 0)
    blank = jnp.zeros((depth - 3 * features - 16, piece), jnp.float32)

    def norms(x, first):
        result = jnp.zeros((8, piece), jnp.float32)
        for k, value in enumerate(three_parts(SCALE * jnp.sum(x * x, axis=0, keepdims=True))):
            result = jnp.where(at == first + k, value, result)
        return result

    def make_rows(j, block):
        x = block.astype(jnp.float32)
        lanes = jnp.concatenate(
            [-2.0 * value for value in three_parts(SCALE * x)] + [ones, norms(x, 0), blank], axis=0)
        rows_x[j * piece : (j + 1) * piece] = lanes.T.astype(jnp.bfloat16)

    def make_cols(slot):
        block = feat[slot]
        tail = jnp.concatenate([norms(block.astype(jnp.float32), 0), ones, blank], axis=0)
        cols_x[slot] = jnp.concatenate([block] * 3 + [tail.astype(jnp.bfloat16)], axis=0)

    def at_rows(j):
        return slice(j * piece, (j + 1) * piece)

    def tiles(rows, slots):
        for slot in slots:
            for j in rows:
                dist = jnp.dot(rows_x[at_rows(j), :], cols_x[slot], preferred_element_type=jnp.float32)
                kmat[at_rows(j), at_rows(slot)] = matern(dist)

    z_near = [0] + z_far[::-1]

    def next_rows(j, slots):
        q = z_near[j]
        copy(feat_z.at[q], feat_z.at[q], fzs.at[q], fzr.at[q], along(q)).wait_recv()
        make_rows(j, feat_z[q])
        tiles([j], slots)

    make_rows(0, feat[0])
    make_cols(0)
    tiles([0], [0])
    feat_arrived(chips)
    make_cols(chips)
    tiles([0], [chips])
    have_rows, have_cols = 1, [0, chips]
    for step in range(max(chips, nw)):
        if have_rows < nw:
            next_rows(have_rows, have_cols)
            have_rows += 1
        new = chips_near[: -1] if step == 0 else chips_near[-1:] if step == 1 else []
        for k in new:
            relay_feat(k)
        for k in new:
            make_cols(k)
            tiles(range(have_rows), [k])
            have_cols.append(k)
    every = range(nw)
    for k in chips_near:
        feat_arrived(chips + k)
        make_cols(chips + k)
        tiles(every, [chips + k])
        relay_dir(k)

    def product_a(j):
        total = None
        for slot in range(nb):
            term = lax.dot_general(kmat[at_rows(j), at_rows(slot)], dir_a[slot], (((1,), (1,)), ((), ())),
                                   preferred_element_type=jnp.float32)
            total = term if total is None else total + term
        return total.T

    def product_b(slot):
        total = None
        for j in every:
            term = jnp.dot(dir_b[z_near[j]], kmat[at_rows(j), at_rows(slot)],
                           preferred_element_type=jnp.float32)
            total = term if total is None else total + term
        return total

    def send_a(j):
        q = z_near[j]
        part_a[j] = product_a(j).astype(jnp.bfloat16)
        go(copy(part_a.at[j], part_a_in.at[nw - q], qs.at[j], qr.at[nw - q], along(q)))

    def send_b(k, c):
        slot = c * chips + k
        to = (other_chip(k) * 2 + (1 - core if c else core), w)
        part_b[slot] = product_b(slot).astype(jnp.bfloat16)
        go(copy(part_b.at[slot], part_b_in.at[slot], ts.at[slot], tr.at[slot], to))

    for k in range(chips):
        dir_arrived(chips + k)
    send_a(nw - 1)
    for q in z_near[1:]:
        copy(dir_b.at[q], dir_b.at[q], bs.at[q], br.at[q], along(q)).wait_recv()
    for at_k, k in enumerate(chips_far):
        for c in range(2):
            send_b(k, c)
        if nw - 2 - at_k > 0:
            send_a(nw - 2 - at_k)
    for j in range(nw - 1 - len(chips_far) - 1, 0, -1):
        send_a(j)
    send_b(0, 1)
    total_a, total_b = product_a(0), product_b(0)
    for q in z_near[1:]:
        copy(part_a_in.at[q], part_a_in.at[q], qs.at[0], qr.at[q], along(q)).wait_recv()
        total_a = total_a + part_a_in[q].astype(jnp.float32)
    for slot in range(1, nb):
        copy(part_b_in.at[slot], part_b_in.at[slot], ts.at[0], tr.at[slot], sibling).wait_recv()
        total_b = total_b + part_b_in[slot].astype(jnp.float32)
    res, direc = residual[...], direction[...]
    total = jnp.concatenate([total_a, total_b], axis=0).T + noise_in[0, 0] * direc

    for k, value in enumerate((res * res, direc * total, res * total, total * total)):
        stat[k : k + 1] = jnp.sum(value, axis=0, keepdims=True)
    for r, q in enumerate(z_far + [0]):
        for k in chips_far + [0]:
            for c in range(2):
                if r == nw - 1 and k == 0 and c == 0:
                    continue
                to = (other_chip(k) * 2 + (core if c == 0 else 1 - core), lax.rem(w + q, nw))
                slot = (lax.rem(nw - q, nw) * 2 + c) * chips + k
                go(copy(stat, stat_in.at[slot], ss.at[0], sr.at[0], to))
    others = stat_in.at[pl.ds(1, nb * nw - 1)]
    copy(others, others, ss.at[0], sr.at[0], sibling).wait_recv()
    sums = stat[...]
    for slot in range(1, nb * nw):
        sums = sums + stat_in[slot]
    old_norm, step = sums[0:1], sums[0:1] / sums[1:2]
    new_norm = old_norm - 2.0 * step * sums[2:3] + step * step * sums[3:4]
    new_residual = res - step * total
    residual_out[...] = new_residual
    solution_out[...] = old_solution[...] + step * direc
    direction_out[...] = new_residual + new_norm / old_norm * direc
    for c in sends[: len(sends) - (nb * nw - 1)]:
        c.wait_send()
    copy(others, others, ss.at[0], sr.at[0], sibling).wait_send()


def long_kernel(nb, nw, points_in, inv_in, noise_in, residual_in, direction_in, solution_in, solution_out, residual_out, direction_out,
           points, inv_length, noise_var, residual, direction, old_solution, io, feat, feat_z, rows_x, kmat, low_dir, part, part_in, stat, stat_z, stat_b, stat_o,
           fs, fr, fzs, fzr, ps, pr, qs, qr, zs, zr, bs, br):
    b = lax.axis_index("blk")
    w = lax.axis_index("wide")
    chips = nb // 2
    chip, core = b // 2, b % 2
    features, piece = points.shape

    def same_core(q):
        return (lax.rem(chip + q, chips) * 2 + core, w)

    sibling = (chip * 2 + 1 - core, w)

    def along(q):
        return (b, lax.rem(w + q, nw))

    def plane(slot):
        return (lax.rem(chip + slot // 2, chips) * 2 + (core if slot % 2 == 0 else 1 - core), w)

    def back(slot):
        return (chips - slot // 2) % chips * 2 + slot % 2

    barrier = pltpu.get_barrier_semaphore()
    for slot in range(1, nb):
        pl.semaphore_signal(barrier, inc=1, device_id=plane(slot), device_id_type=MESH)
    for q in range(1, nw):
        pl.semaphore_signal(barrier, inc=1, device_id=along(q), device_id_type=MESH)

    def copy(src, dst, send, recv, to):
        return pltpu.make_async_remote_copy(
            src_ref=src, dst_ref=dst, send_sem=send, recv_sem=recv, device_id=to, device_id_type=MESH
        )

    loads = [
        pltpu.make_async_copy(src, dst, io.at[k])
        for k, (src, dst) in enumerate(
            ((points_in, points), (inv_in, inv_length), (direction_in, direction),
             (residual_in, residual), (solution_in, old_solution))
        )
    ]
    for load in loads:
        load.start()
    for load in loads[:2]:
        load.wait()

    inv_row = jnp.concatenate(
        [inv_length[...], jnp.zeros((1, 128 - features), jnp.float32)], axis=1)
    inv_column = jnp.broadcast_to(inv_row, (8, 128)).T[:features, 0:1]
    x_t = rounded(points[...].astype(jnp.float32) * inv_column)
    s1, s2, s3 = three_parts(SCALE * jnp.sum(x_t * x_t, axis=0, keepdims=True))
    row = lax.broadcasted_iota(jnp.int32, (TAIL, piece), 0)
    tail = jnp.where((row >= 3) & (row <= 10), 1.0, 0.0)
    tail = jnp.where((row >= 6) & (row <= 7), 0.0, tail)
    for at, value in ((0, s1), (1, s2), (2, s3), (11, s1), (12, s2), (13, s3)):
        tail = jnp.where(row == at, value, tail)
    feat[0] = jnp.concatenate([x_t, tail], axis=0).astype(jnp.bfloat16)
    for load in loads[2:]:
        load.wait()
    low_dir[0:piece] = direction[...].astype(jnp.bfloat16)
    pl.semaphore_wait(barrier, nb - 1 + nw - 1)

    upper = lax.div(2 * w, nw)

    def near(k):
        return k + upper * (nw - 2 * k)

    def rows_at(q):
        return pl.ds(pl.multiple_of(q * piece, piece), piece)

    sends = []

    def go(c):
        c.start()
        sends.append(c)
        return c

    def feat_copy(src_slot, dst_slot, to):
        return copy(feat.at[src_slot], feat.at[dst_slot], fs.at[dst_slot], fr.at[dst_slot], to)

    def dir_copy(src_slot, dst_slot, to):
        return copy(low_dir.at[pl.ds(src_slot * piece, piece)], low_dir.at[pl.ds(dst_slot * piece, piece)],
                    ps.at[dst_slot], pr.at[dst_slot], to)

    for k in range(1, nw):
        q = near(nw - k)
        go(copy(feat.at[0], feat_z.at[nw - q], fzs.at[q], fzr.at[nw - q], along(q)))
    go(feat_copy(0, 1, sibling))
    for q in range(1, chips):
        go(feat_copy(0, 2 * (chips - q), same_core(q)))
    for q in range(1, chips):
        go(dir_copy(0, 2 * (chips - q), same_core(q)))
    go(dir_copy(0, 1, sibling))

    def feat_arrived(slot):
        feat_copy(slot, slot, sibling).wait_recv()

    def dir_arrived(slot):
        dir_copy(slot, slot, sibling).wait_recv()

    def as_rows(block):
        block = block.astype(jnp.float32)
        x = block[:features]
        h, m, l = three_parts(SCALE * x)
        lanes = jnp.concatenate(
            [-2.0 * h, -2.0 * m, -2.0 * l, block[features + 8 :],
             jnp.zeros((TAIL + 8, piece), jnp.float32)], axis=0)
        return lanes.T.astype(jnp.bfloat16)

    depth = rows_x.shape[1]

    def tile(at, slot):
        block = feat[slot]
        cols = jnp.concatenate(
            [block[:features]] * 3 + [block[features:],
             jnp.zeros((depth - 3 * features - TAIL, piece), jnp.bfloat16)], axis=0)
        dist = jnp.dot(rows_x[at, :], cols, preferred_element_type=jnp.float32)
        kmat[at, slot * piece : (slot + 1) * piece] = matern(dist)

    def feat_z_arrived(q):
        copy(feat_z.at[q], feat_z.at[q], fzs.at[q], fzr.at[q], along(q)).wait_recv()

    def relay_direction(q):
        dir_arrived(2 * q)
        go(dir_copy(2 * q, 2 * q + 1, sibling))

    rows_x[0:piece] = as_rows(feat[0])
    tile(pl.ds(0, piece), 0)
    feat_arrived(1)
    tile(pl.ds(0, piece), 1)
    for q in range(1, chips):
        feat_arrived(2 * q)
        go(feat_copy(2 * q, 2 * q + 1, sibling))
        tile(pl.ds(0, piece), 2 * q)
    for q in range(1, chips):
        feat_arrived(2 * q + 1)
        tile(pl.ds(0, piece), 2 * q + 1)
    if nw <= 4:
        relayed = 1
        for k in range(1, nw):
            q = near(k)
            feat_z_arrived(q)
            rows_x[rows_at(q), :] = as_rows(feat_z[q])
            for slot in range(nb):
                tile(rows_at(q), slot)
                if k == nw - 1 and slot in (0, nb // 2) and relayed < chips:
                    relay_direction(relayed)
                    relayed += 1
    else:
        relayed = 1
        for q in range(1, nw):
            feat_z_arrived(q)
            rows_x[q * piece : (q + 1) * piece] = as_rows(feat_z[q])

        def row_tiles(q, carry):
            for slot in range(nb):
                tile(pl.ds(pl.multiple_of(q * piece, piece), piece), slot)
            return carry

        lax.fori_loop(1, nw, row_tiles, 0)
    for q in range(relayed, chips):
        relay_direction(q)
    for q in range(chips):
        dir_arrived(2 * q + 1)

    def partial(q):
        return jnp.dot(kmat[rows_at(q), :], low_dir[...],
                       preferred_element_type=jnp.float32)

    for k in range(1, nw):
        q = near(nw - k)
        part[q] = partial(q).astype(jnp.bfloat16)
        go(copy(part.at[q], part_in.at[nw - q], qs.at[q], qr.at[nw - q], along(q)))
    total = partial(0) + noise_in[0, 0] * direction[...]
    for q in range(1, nw):
        copy(part.at[q], part_in.at[q], qs.at[q], qr.at[q], along(q)).wait_recv()
        total = total + part_in[q].astype(jnp.float32)

    def column_sum(x):
        return jnp.sum(x, axis=0, keepdims=True)

    res, direc = residual[...], direction[...]
    at = lax.broadcasted_iota(jnp.int32, (8, res.shape[1]), 0)
    sums = jnp.zeros(at.shape, jnp.float32)
    for k, value in enumerate((res * res, direc * total, res * total, total * total)):
        sums = jnp.where(at == k, column_sum(value), sums)
    stat[...] = sums
    for q in range(1, nw):
        go(copy(stat, stat_z.at[nw - q], zs.at[q], zr.at[nw - q], along(q)))
    for q in range(1, nw):
        copy(stat, stat_z.at[q], zs.at[q], zr.at[q], along(q)).wait_recv()
        sums = sums + stat_z[q]
    stat_o[...] = sums
    for slot in range(1, nb):
        go(copy(stat_o, stat_b.at[back(slot)], bs.at[slot], br.at[back(slot)], plane(slot)))
    for slot in range(1, nb):
        copy(stat_o, stat_b.at[slot], bs.at[slot], br.at[slot], plane(slot)).wait_recv()
        sums = sums + stat_b[slot]
    old_norm, step = sums[0:1], sums[0:1] / sums[1:2]
    new_norm = old_norm - 2.0 * step * sums[2:3] + step * step * sums[3:4]
    new_residual = res - step * total
    residual_out[...] = new_residual
    solution_out[...] = old_solution[...] + step * direc
    direction_out[...] = new_residual + new_norm / old_norm * direc
    for c in sends:
        c.wait_send()


def write_out(a, b, c, a_out, b_out, c_out, sems):
    copies = [
        pltpu.make_async_copy(src, dst, sems.at[k])
        for k, (src, dst) in enumerate(((a, a_out), (b, b_out), (c, c_out)))
    ]
    for copy in copies:
        copy.start()
    for copy in copies:
        copy.wait()


def on_device(nb, nw, points, inv_length, noise_var, solution, residual, direction):
    piece, features = points.shape
    rhs = direction.shape[1]
    vmem = pl.BlockSpec(memory_space=pltpu.VMEM)
    hbm = pl.BlockSpec(memory_space=pl.ANY)
    dma = pltpu.SemaphoreType.DMA
    depth = 3 * features + 2 * TAIL
    common = [
        pltpu.VMEM((features, piece), points.dtype),
        pltpu.VMEM((1, features), jnp.float32),
    ]
    wide = [
        dma((6,)),
        pltpu.VMEM((nb, features + TAIL, piece), jnp.bfloat16),
        pltpu.VMEM((nw, features + TAIL, piece), jnp.bfloat16),
        pltpu.VMEM((nw * piece, depth), jnp.bfloat16),
        pltpu.VMEM((nw * piece, nb * piece), jnp.bfloat16),
        pltpu.VMEM((nb * piece, rhs), jnp.bfloat16),
    ]
    vectors = [pltpu.VMEM((piece, rhs), jnp.float32)] * 3
    parts = [pltpu.VMEM((nw, piece, rhs), jnp.bfloat16)] * 2
    sems = [dma((nb,)), dma((nb,)), dma((nw,)), dma((nw,)), dma((nb,)), dma((nb,)), dma((nw,)), dma((nw,))]
    if nw <= 4:
        body = kernel
        half = rhs // 2
        low = jnp.bfloat16
        scratch = common + vectors + [
            dma((6,)),
            pltpu.VMEM((nb, features, piece), low), pltpu.VMEM((nw, features, piece), low),
            pltpu.VMEM((nw * piece, depth), low), pltpu.VMEM((nb, depth, piece), low),
            pltpu.VMEM((nw * piece, nb * piece), low),
            pltpu.VMEM((nb, half, piece), low), pltpu.VMEM((nw, half, piece), low),
            pltpu.VMEM((nw, half, piece), low), pltpu.VMEM((nw, half, piece), low),
            pltpu.VMEM((nb, half, piece), low), pltpu.VMEM((nb, half, piece), low),
            pltpu.VMEM((4, rhs), jnp.float32), pltpu.VMEM((nw * nb, 4, rhs), jnp.float32),
        ] + sems + [dma((nw,)), dma((nw,)), dma((nb,)), dma((nb,)), dma((1,)), dma((1,))]
    else:
        body = long_kernel
        scratch = common + [pltpu.VMEM((1, 1), jnp.float32)] + vectors + wide + parts + [
            pltpu.VMEM((8, rhs), jnp.float32),
            pltpu.VMEM((nw, 8, rhs), jnp.float32),
            pltpu.VMEM((nb, 8, rhs), jnp.float32),
            pltpu.VMEM((8, rhs), jnp.float32),
        ] + sems + [dma((nw,)), dma((nw,)), dma((nb,)), dma((nb,))]
    news = pl.pallas_call(
        functools.partial(body, nb, nw),
        out_shape=(pltpu.VMEM((piece, rhs), jnp.float32),) * 3,
        in_specs=[hbm, hbm, pl.BlockSpec(memory_space=pltpu.SMEM), hbm, hbm, hbm],
        out_specs=(vmem,) * 3,
        scratch_shapes=scratch,
        compiler_params=pltpu.CompilerParams(
            collective_id=0, has_side_effects=True, vmem_limit_bytes=60 * 1024 * 1024
        ),
    )(points.T, inv_length.reshape(1, features), noise_var.reshape(1, 1), residual, direction, solution)
    return pl.pallas_call(
        write_out,
        out_shape=(jax.ShapeDtypeStruct((piece, rhs), jnp.float32),) * 3,
        in_specs=[vmem] * 3,
        out_specs=(hbm,) * 3,
        scratch_shapes=[dma((3,))],
    )(*(pltpu.with_memory_space_constraint(x, pltpu.VMEM) for x in news))


def solution(mesh):
    spec = P(("blk", "wide"), None)
    return jax.shard_map(
        functools.partial(on_device, mesh.shape["blk"], mesh.shape["wide"]),
        mesh=mesh,
        in_specs=(spec, P(), P(), spec, spec, spec),
        out_specs=(spec, spec, spec),
        check_vma=False,
    )
```

```python
import functools
import math

import jax
import jax.numpy as jnp
from jax import lax
from jax.experimental import pallas as pl
from jax.experimental.pallas import tpu as pltpu
from jax.sharding import PartitionSpec as P

LN2 = math.log(2.0)
SCALE = 5.0 / (LN2 * LN2)
MESH = pl.DeviceIdType.MESH
TAIL = 16


def rounded(x):
    return x.astype(jnp.bfloat16).astype(jnp.float32)


def three_parts(x):
    high = rounded(x)
    rest = x - high
    middle = rounded(rest)
    return high, middle, rounded(rest - middle)


def matern(scaled_dist):
    dist = jnp.maximum(scaled_dist, 1e-30)
    root = dist * lax.rsqrt(dist)
    poly = 1.0 + root * (LN2 + (LN2 * LN2 / 3.0) * root)
    return (poly * jnp.exp2(-root)).astype(jnp.bfloat16)


def kernel(nb, nw, points_in, inv_in, noise_in, residual_in, direction_in, solution_in, solution_out, residual_out, direction_out,
           points, inv_length, direction, others, io, feat, feat_z, rows_x, cols_x, kmat, dir_a, dir_b, dir_rows, part_a, part_a_in, part_b, part_b_in, stat, stat_in,
           sent, feat_sem, feat_z_sem, dir_sem, got):
    b = lax.axis_index("blk")
    w = lax.axis_index("wide")
    chips = nb // 2
    chip, core = b // 2, b % 2
    features, piece = points.shape

    def other_chip(k):
        at, bit = chip, 1
        while bit < chips:
            if k & bit:
                at = at + bit - 2 * bit * lax.rem(lax.div(chip, bit), 2)
            bit *= 2
        return at

    def same_core(k):
        return (other_chip(k) * 2 + core, w)

    sibling = (chip * 2 + 1 - core, w)

    def along(q):
        return (b, lax.rem(w + q, nw))

    def at_least(limit):
        return lax.div(w + nw - limit, nw)

    upper = lax.div(2 * w, nw)

    def far_first(k):
        low = nw - 1 - k - at_least(nw - 1 - k)
        high = k + 1 - at_least(k + 1)
        return lax.rem(low + upper * (high - low) - w + nw, nw)

    z_far = [far_first(k) for k in range(nw - 1)]
    chips_far = sorted(range(1, chips), key=lambda k: -bin(k).count("1"))
    chips_near = chips_far[::-1]

    barrier = pltpu.get_barrier_semaphore()
    for k in range(1, chips):
        pl.semaphore_signal(barrier, inc=1, device_id=same_core(k), device_id_type=MESH)
    pl.semaphore_signal(barrier, inc=1, device_id=sibling, device_id_type=MESH)
    for q in range(1, nw):
        pl.semaphore_signal(barrier, inc=1, device_id=along(q), device_id_type=MESH)

    def copy(src, dst, send, recv, to):
        return pltpu.make_async_remote_copy(
            src_ref=src, dst_ref=dst, send_sem=send, recv_sem=recv, device_id=to, device_id_type=MESH
        )

    loads = [
        pltpu.make_async_copy(src, dst, io.at[min(k, 3)])
        for k, (src, dst) in enumerate(
            ((points_in, points), (inv_in, inv_length), (direction_in, direction),
             (residual_in, others.at[0]), (solution_in, others.at[1]))
        )
    ]
    for load in loads:
        load.start()
    for load in loads[:2]:
        load.wait()

    inv_row = jnp.concatenate(
        [inv_length[...], jnp.zeros((1, 128 - features), jnp.float32)], axis=1)
    inv_column = jnp.broadcast_to(inv_row, (8, 128)).T[:features, 0:1]
    x_t = rounded(points[...].astype(jnp.float32) * inv_column)
    feat[0] = x_t.astype(jnp.bfloat16)
    pl.semaphore_wait(barrier, chips + nw - 1)

    FEAT, FEAT_Z, DIR, DIR_Z, PART, PART_Z, STAT = range(7)

    def feat_copy(src_slot, dst_slot, to):
        return copy(feat.at[src_slot], feat.at[dst_slot], sent.at[FEAT], feat_sem.at[dst_slot - 1], to)

    def dir_copy(src_slot, dst_slot, to):
        return copy(dir_a.at[src_slot], dir_a.at[dst_slot], sent.at[DIR], dir_sem.at[min(dst_slot, chips) - 1], to)

    def feat_z_copy(src, slot, q):
        return copy(src, feat_z.at[slot], sent.at[FEAT_Z], feat_z_sem.at[slot - 1], along(q))

    for q in z_far:
        feat_z_copy(feat.at[0], nw - q, q).start()
    for k in chips_far:
        feat_copy(0, k, same_core(k)).start()
    feat_copy(0, chips, sibling).start()
    loads[2].wait()
    dir_t = direction[...].T.astype(jnp.bfloat16)
    part = dir_t.shape[0] // 2
    dir_a[0] = dir_t[:part]
    dir_b[0] = dir_t[part:]
    for k in chips_far:
        dir_copy(0, k, same_core(k)).start()
    dir_copy(0, chips, sibling).start()
    dir_rows[0:piece] = direction[...][:, :part].astype(jnp.bfloat16)

    def feat_arrived(slot):
        feat_copy(slot, slot, sibling).wait_recv()

    def relay_feat(k):
        feat_arrived(k)
        feat_copy(k, chips + k, sibling).start()

    def turn(slot):
        dir_rows[at_rows(slot), :] = dir_a[slot].astype(jnp.float32).T.astype(jnp.bfloat16)

    def relay_dir(k):
        dir_copy(k, k, sibling).wait_recv()
        dir_copy(k, chips + k, sibling).start()

    depth = rows_x.shape[1]
    ones = jnp.where(lax.broadcasted_iota(jnp.int32, (8, piece), 0) < 3, 1.0, 0.0)
    at = lax.broadcasted_iota(jnp.int32, (8, piece), 0)
    blank = jnp.zeros((depth - 3 * features - 16, piece), jnp.float32)

    def norms(x, first):
        result = jnp.zeros((8, piece), jnp.float32)
        for k, value in enumerate(three_parts(SCALE * jnp.sum(x * x, axis=0, keepdims=True))):
            result = jnp.where(at == first + k, value, result)
        return result

    def make_rows(j, block):
        x = block.astype(jnp.float32)
        lanes = jnp.concatenate(
            [-2.0 * value for value in three_parts(SCALE * x)] + [ones, norms(x, 0), blank], axis=0)
        rows_x[j * piece : (j + 1) * piece] = lanes.T.astype(jnp.bfloat16)

    def make_cols(slot):
        block = feat[slot]
        tail = jnp.concatenate([norms(block.astype(jnp.float32), 0), ones, blank], axis=0)
        cols_x[slot] = jnp.concatenate([block] * 3 + [tail.astype(jnp.bfloat16)], axis=0)

    def at_rows(j):
        return slice(j * piece, (j + 1) * piece)

    def tiles(rows, slots):
        for slot in slots:
            for j in rows:
                dist = jnp.dot(rows_x[at_rows(j), :], cols_x[slot], preferred_element_type=jnp.float32)
                kmat[at_rows(j), at_rows(slot)] = matern(dist)

    z_near = [0] + z_far[::-1]

    have_rows, have_cols = [], []

    def add_rows(j):
        if j:
            q = z_near[j]
            feat_z_copy(feat_z.at[q], q, q).wait_recv()
            make_rows(j, feat_z[q])
        else:
            make_rows(0, feat[0])
        tiles([j], have_cols)
        have_rows.append(j)

    def add_cols(slot):
        if slot >= chips:
            feat_arrived(slot)
        make_cols(slot)
        tiles(have_rows, [slot])
        have_cols.append(slot)

    every = range(nw)
    near, last = chips_near[:-1], chips_near[-1:]
    add_rows(0)
    add_cols(0)
    add_cols(chips)
    for q in z_far:
        copy(dir_b.at[0], dir_b.at[nw - q], sent.at[DIR_Z], got.at[DIR_Z], along(q)).start()
    for k in near:
        relay_feat(k)
    for k in near:
        add_cols(k)
    if nw > 1:
        add_rows(1)
    for k in last:
        relay_feat(k)
        add_cols(k)
    for k in near:
        add_cols(chips + k)
    for j in range(2, nw - 1):
        add_rows(j)
    for k in near:
        relay_dir(k)
    for j in range(max(2, nw - 1), nw):
        add_rows(j)
    for k in last:
        relay_dir(k)
    for k in range(1, chips):
        turn(k)
    for k in last:
        add_cols(chips + k)

    def product_a(j):
        return jnp.dot(kmat[at_rows(j), :], dir_rows[...], preferred_element_type=jnp.float32).T

    def product_b(slot):
        total = None
        for j in every:
            term = jnp.dot(dir_b[z_near[j]], kmat[at_rows(j), at_rows(slot)],
                           preferred_element_type=jnp.float32)
            total = term if total is None else total + term
        return total

    def send_a(j):
        q = z_near[j]
        part_a[j] = product_a(j).astype(jnp.bfloat16)
        copy(part_a.at[j], part_a_in.at[nw - q], sent.at[PART_Z], got.at[PART_Z], along(q)).start()

    def send_b(k, c):
        slot = c * chips + k
        to = (other_chip(k) * 2 + (1 - core if c else core), w)
        part_b[slot] = product_b(slot).astype(jnp.bfloat16)
        copy(part_b.at[slot], part_b_in.at[slot], sent.at[PART], got.at[PART], to).start()

    def all_of(ref, kind, recv):
        return copy(ref, ref, sent.at[kind], recv, sibling)

    relayed, z_dirs = dir_a.at[pl.ds(chips, chips)], dir_b.at[pl.ds(1, nw - 1)]
    all_of(relayed, DIR, dir_sem.at[chips - 1]).wait_recv()
    for k in range(chips):
        turn(chips + k)
    send_a(nw - 1)
    all_of(z_dirs, DIR_Z, got.at[DIR_Z]).wait_recv()
    for at_k, k in enumerate(chips_far):
        for c in range(2):
            send_b(k, c)
        if nw - 2 - at_k > 0:
            send_a(nw - 2 - at_k)
    for j in range(nw - 1 - len(chips_far) - 1, 0, -1):
        send_a(j)
    send_b(0, 1)
    total_a, total_b = product_a(0), product_b(0)
    parts_z, parts_b = part_a_in.at[pl.ds(1, nw - 1)], part_b_in.at[pl.ds(1, nb - 1)]
    all_of(parts_z, PART_Z, got.at[PART_Z]).wait_recv()
    for q in range(1, nw):
        total_a = total_a + part_a_in[q].astype(jnp.float32)
    all_of(parts_b, PART, got.at[PART]).wait_recv()
    for slot in range(1, nb):
        total_b = total_b + part_b_in[slot].astype(jnp.float32)
    make_vectors = pltpu.make_async_copy(others, others, io.at[3])
    make_vectors.wait()
    res, direc = others[0], direction[...]
    total = jnp.concatenate([total_a, total_b], axis=0).T + noise_in[0, 0] * direc

    for k, value in enumerate((res * res, direc * total, res * total, total * total)):
        stat[k : k + 1] = jnp.sum(value, axis=0, keepdims=True)
    for r, q in enumerate(z_far + [0]):
        for k in chips_far + [0]:
            for c in range(2):
                if r == nw - 1 and k == 0 and c == 0:
                    continue
                to = (other_chip(k) * 2 + (core if c == 0 else 1 - core), lax.rem(w + q, nw))
                slot = (lax.rem(nw - q, nw) * 2 + c) * chips + k
                copy(stat, stat_in.at[slot], sent.at[STAT], got.at[STAT], to).start()
    stats = stat_in.at[pl.ds(1, nb * nw - 1)]
    all_of(stats, STAT, got.at[STAT]).wait_recv()
    sums = stat[...]
    for slot in range(1, nb * nw):
        sums = sums + stat_in[slot]
    old_norm, step = sums[0:1], sums[0:1] / sums[1:2]
    new_norm = old_norm - 2.0 * step * sums[2:3] + step * step * sums[3:4]
    new_residual = res - step * total
    residual_out[...] = new_residual
    solution_out[...] = others[1] + step * direc
    direction_out[...] = new_residual + new_norm / old_norm * direc
    for ref, kind in ((feat.at[pl.ds(1, nb - 1)], FEAT), (feat_z.at[pl.ds(1, nw - 1)], FEAT_Z), (dir_a.at[pl.ds(1, nb - 1)], DIR),
                      (z_dirs, DIR_Z), (parts_b, PART), (parts_z, PART_Z), (stats, STAT)):
        all_of(ref, kind, got.at[kind]).wait_send()


def long_kernel(nb, nw, points_in, inv_in, noise_in, residual_in, direction_in, solution_in, solution_out, residual_out, direction_out,
           points, inv_length, noise_var, residual, direction, old_solution, io, feat, feat_z, rows_x, kmat, low_dir, part, part_in, stat, stat_z, stat_b, stat_o,
           fs, fr, fzs, fzr, ps, pr, qs, qr, zs, zr, bs, br):
    b = lax.axis_index("blk")
    w = lax.axis_index("wide")
    chips = nb // 2
    chip, core = b // 2, b % 2
    features, piece = points.shape

    def same_core(q):
        return (lax.rem(chip + q, chips) * 2 + core, w)

    sibling = (chip * 2 + 1 - core, w)

    def along(q):
        return (b, lax.rem(w + q, nw))

    def plane(slot):
        return (lax.rem(chip + slot // 2, chips) * 2 + (core if slot % 2 == 0 else 1 - core), w)

    def back(slot):
        return (chips - slot // 2) % chips * 2 + slot % 2

    barrier = pltpu.get_barrier_semaphore()
    for slot in range(1, nb):
        pl.semaphore_signal(barrier, inc=1, device_id=plane(slot), device_id_type=MESH)
    for q in range(1, nw):
        pl.semaphore_signal(barrier, inc=1, device_id=along(q), device_id_type=MESH)

    def copy(src, dst, send, recv, to):
        return pltpu.make_async_remote_copy(
            src_ref=src, dst_ref=dst, send_sem=send, recv_sem=recv, device_id=to, device_id_type=MESH
        )

    loads = [
        pltpu.make_async_copy(src, dst, io.at[k])
        for k, (src, dst) in enumerate(
            ((points_in, points), (inv_in, inv_length), (direction_in, direction),
             (residual_in, residual), (solution_in, old_solution))
        )
    ]
    for load in loads:
        load.start()
    for load in loads[:2]:
        load.wait()

    inv_row = jnp.concatenate(
        [inv_length[...], jnp.zeros((1, 128 - features), jnp.float32)], axis=1)
    inv_column = jnp.broadcast_to(inv_row, (8, 128)).T[:features, 0:1]
    x_t = rounded(points[...].astype(jnp.float32) * inv_column)
    s1, s2, s3 = three_parts(SCALE * jnp.sum(x_t * x_t, axis=0, keepdims=True))
    row = lax.broadcasted_iota(jnp.int32, (TAIL, piece), 0)
    tail = jnp.where((row >= 3) & (row <= 10), 1.0, 0.0)
    tail = jnp.where((row >= 6) & (row <= 7), 0.0, tail)
    for at, value in ((0, s1), (1, s2), (2, s3), (11, s1), (12, s2), (13, s3)):
        tail = jnp.where(row == at, value, tail)
    feat[0] = jnp.concatenate([x_t, tail], axis=0).astype(jnp.bfloat16)
    for load in loads[2:]:
        load.wait()
    low_dir[0:piece] = direction[...].astype(jnp.bfloat16)
    pl.semaphore_wait(barrier, nb - 1 + nw - 1)

    upper = lax.div(2 * w, nw)

    def near(k):
        return k + upper * (nw - 2 * k)

    def rows_at(q):
        return pl.ds(pl.multiple_of(q * piece, piece), piece)

    sends = []

    def go(c):
        c.start()
        sends.append(c)
        return c

    def feat_copy(src_slot, dst_slot, to):
        return copy(feat.at[src_slot], feat.at[dst_slot], fs.at[dst_slot], fr.at[dst_slot], to)

    def dir_copy(src_slot, dst_slot, to):
        return copy(low_dir.at[pl.ds(src_slot * piece, piece)], low_dir.at[pl.ds(dst_slot * piece, piece)],
                    ps.at[dst_slot], pr.at[dst_slot], to)

    for k in range(1, nw):
        q = near(nw - k)
        go(copy(feat.at[0], feat_z.at[nw - q], fzs.at[q], fzr.at[nw - q], along(q)))
    go(feat_copy(0, 1, sibling))
    for q in range(1, chips):
        go(feat_copy(0, 2 * (chips - q), same_core(q)))
    for q in range(1, chips):
        go(dir_copy(0, 2 * (chips - q), same_core(q)))
    go(dir_copy(0, 1, sibling))

    def feat_arrived(slot):
        feat_copy(slot, slot, sibling).wait_recv()

    def dir_arrived(slot):
        dir_copy(slot, slot, sibling).wait_recv()

    def as_rows(block):
        block = block.astype(jnp.float32)
        x = block[:features]
        h, m, l = three_parts(SCALE * x)
        lanes = jnp.concatenate(
            [-2.0 * h, -2.0 * m, -2.0 * l, block[features + 8 :],
             jnp.zeros((TAIL + 8, piece), jnp.float32)], axis=0)
        return lanes.T.astype(jnp.bfloat16)

    depth = rows_x.shape[1]

    def tile(at, slot):
        block = feat[slot]
        cols = jnp.concatenate(
            [block[:features]] * 3 + [block[features:],
             jnp.zeros((depth - 3 * features - TAIL, piece), jnp.bfloat16)], axis=0)
        dist = jnp.dot(rows_x[at, :], cols, preferred_element_type=jnp.float32)
        kmat[at, slot * piece : (slot + 1) * piece] = matern(dist)

    def feat_z_arrived(q):
        copy(feat_z.at[q], feat_z.at[q], fzs.at[q], fzr.at[q], along(q)).wait_recv()

    def relay_direction(q):
        dir_arrived(2 * q)
        go(dir_copy(2 * q, 2 * q + 1, sibling))

    rows_x[0:piece] = as_rows(feat[0])
    tile(pl.ds(0, piece), 0)
    feat_arrived(1)
    tile(pl.ds(0, piece), 1)
    for q in range(1, chips):
        feat_arrived(2 * q)
        go(feat_copy(2 * q, 2 * q + 1, sibling))
        tile(pl.ds(0, piece), 2 * q)
    for q in range(1, chips):
        feat_arrived(2 * q + 1)
        tile(pl.ds(0, piece), 2 * q + 1)
    if nw <= 4:
        relayed = 1
        for k in range(1, nw):
            q = near(k)
            feat_z_arrived(q)
            rows_x[rows_at(q), :] = as_rows(feat_z[q])
            for slot in range(nb):
                tile(rows_at(q), slot)
                if k == nw - 1 and slot in (0, nb // 2) and relayed < chips:
                    relay_direction(relayed)
                    relayed += 1
    else:
        relayed = 1
        for q in range(1, nw):
            feat_z_arrived(q)
            rows_x[q * piece : (q + 1) * piece] = as_rows(feat_z[q])

        def row_tiles(q, carry):
            for slot in range(nb):
                tile(pl.ds(pl.multiple_of(q * piece, piece), piece), slot)
            return carry

        lax.fori_loop(1, nw, row_tiles, 0)
    for q in range(relayed, chips):
        relay_direction(q)
    for q in range(chips):
        dir_arrived(2 * q + 1)

    def partial(q):
        return jnp.dot(kmat[rows_at(q), :], low_dir[...],
                       preferred_element_type=jnp.float32)

    for k in range(1, nw):
        q = near(nw - k)
        part[q] = partial(q).astype(jnp.bfloat16)
        go(copy(part.at[q], part_in.at[nw - q], qs.at[q], qr.at[nw - q], along(q)))
    total = partial(0) + noise_in[0, 0] * direction[...]
    for q in range(1, nw):
        copy(part.at[q], part_in.at[q], qs.at[q], qr.at[q], along(q)).wait_recv()
        total = total + part_in[q].astype(jnp.float32)

    def column_sum(x):
        return jnp.sum(x, axis=0, keepdims=True)

    res, direc = residual[...], direction[...]
    at = lax.broadcasted_iota(jnp.int32, (8, res.shape[1]), 0)
    sums = jnp.zeros(at.shape, jnp.float32)
    for k, value in enumerate((res * res, direc * total, res * total, total * total)):
        sums = jnp.where(at == k, column_sum(value), sums)
    stat[...] = sums
    for q in range(1, nw):
        go(copy(stat, stat_z.at[nw - q], zs.at[q], zr.at[nw - q], along(q)))
    for q in range(1, nw):
        copy(stat, stat_z.at[q], zs.at[q], zr.at[q], along(q)).wait_recv()
        sums = sums + stat_z[q]
    stat_o[...] = sums
    for slot in range(1, nb):
        go(copy(stat_o, stat_b.at[back(slot)], bs.at[slot], br.at[back(slot)], plane(slot)))
    for slot in range(1, nb):
        copy(stat_o, stat_b.at[slot], bs.at[slot], br.at[slot], plane(slot)).wait_recv()
        sums = sums + stat_b[slot]
    old_norm, step = sums[0:1], sums[0:1] / sums[1:2]
    new_norm = old_norm - 2.0 * step * sums[2:3] + step * step * sums[3:4]
    new_residual = res - step * total
    residual_out[...] = new_residual
    solution_out[...] = old_solution[...] + step * direc
    direction_out[...] = new_residual + new_norm / old_norm * direc
    for c in sends:
        c.wait_send()


def write_out(a, b, c, a_out, b_out, c_out, sems):
    copies = [
        pltpu.make_async_copy(src, dst, sems.at[k])
        for k, (src, dst) in enumerate(((a, a_out), (b, b_out), (c, c_out)))
    ]
    for copy in copies:
        copy.start()
    for copy in copies:
        copy.wait()


def on_device(nb, nw, points, inv_length, noise_var, solution, residual, direction):
    piece, features = points.shape
    rhs = direction.shape[1]
    vmem = pl.BlockSpec(memory_space=pltpu.VMEM)
    hbm = pl.BlockSpec(memory_space=pl.ANY)
    dma = pltpu.SemaphoreType.DMA
    depth = 3 * features + 2 * TAIL
    common = [
        pltpu.VMEM((features, piece), points.dtype),
        pltpu.VMEM((1, features), jnp.float32),
    ]
    wide = [
        dma((6,)),
        pltpu.VMEM((nb, features + TAIL, piece), jnp.bfloat16),
        pltpu.VMEM((nw, features + TAIL, piece), jnp.bfloat16),
        pltpu.VMEM((nw * piece, depth), jnp.bfloat16),
        pltpu.VMEM((nw * piece, nb * piece), jnp.bfloat16),
        pltpu.VMEM((nb * piece, rhs), jnp.bfloat16),
    ]
    vectors = [pltpu.VMEM((piece, rhs), jnp.float32)] * 3
    parts = [pltpu.VMEM((nw, piece, rhs), jnp.bfloat16)] * 2
    sems = [dma((nb,)), dma((nb,)), dma((nw,)), dma((nw,)), dma((nb,)), dma((nb,)), dma((nw,)), dma((nw,))]
    if nw <= 4:
        body = kernel
        half = rhs // 2
        low = jnp.bfloat16
        scratch = common + [
            pltpu.VMEM((piece, rhs), jnp.float32), pltpu.VMEM((2, piece, rhs), jnp.float32), dma((4,)),
            pltpu.VMEM((nb, features, piece), low), pltpu.VMEM((nw, features, piece), low),
            pltpu.VMEM((nw * piece, depth), low), pltpu.VMEM((nb, depth, piece), low),
            pltpu.VMEM((nw * piece, nb * piece), low),
            pltpu.VMEM((nb, half, piece), low), pltpu.VMEM((nw, half, piece), low),
            pltpu.VMEM((nb * piece, half), low),
            pltpu.VMEM((nw, half, piece), low), pltpu.VMEM((nw, half, piece), low),
            pltpu.VMEM((nb, half, piece), low), pltpu.VMEM((nb, half, piece), low),
            pltpu.VMEM((4, rhs), jnp.float32), pltpu.VMEM((nw * nb, 4, rhs), jnp.float32),
            dma((7,)), dma((nb - 1,)), dma((nw - 1,)), dma((nb // 2,)), dma((7,)),
        ]
    else:
        body = long_kernel
        scratch = common + [pltpu.VMEM((1, 1), jnp.float32)] + vectors + wide + parts + [
            pltpu.VMEM((8, rhs), jnp.float32),
            pltpu.VMEM((nw, 8, rhs), jnp.float32),
            pltpu.VMEM((nb, 8, rhs), jnp.float32),
            pltpu.VMEM((8, rhs), jnp.float32),
        ] + sems + [dma((nw,)), dma((nw,)), dma((nb,)), dma((nb,))]
    news = pl.pallas_call(
        functools.partial(body, nb, nw),
        out_shape=(pltpu.VMEM((piece, rhs), jnp.float32),) * 3,
        in_specs=[hbm, hbm, pl.BlockSpec(memory_space=pltpu.SMEM), hbm, hbm, hbm],
        out_specs=(vmem,) * 3,
        scratch_shapes=scratch,
        compiler_params=pltpu.CompilerParams(
            collective_id=0, has_side_effects=True, vmem_limit_bytes=60 * 1024 * 1024
        ),
    )(points.T, inv_length.reshape(1, features), noise_var.reshape(1, 1), residual, direction, solution)
    return pl.pallas_call(
        write_out,
        out_shape=(jax.ShapeDtypeStruct((piece, rhs), jnp.float32),) * 3,
        in_specs=[vmem] * 3,
        out_specs=(hbm,) * 3,
        scratch_shapes=[dma((3,))],
    )(*(pltpu.with_memory_space_constraint(x, pltpu.VMEM) for x in news))


def solution(mesh):
    spec = P(("blk", "wide"), None)
    return jax.shard_map(
        functools.partial(on_device, mesh.shape["blk"], mesh.shape["wide"]),
        mesh=mesh,
        in_specs=(spec, P(), P(), spec, spec, spec),
        out_specs=(spec, spec, spec),
        check_vma=False,
    )
```

```python
import functools
import math

import jax
import jax.numpy as jnp
from jax import lax
from jax.experimental import pallas as pl
from jax.experimental.pallas import tpu as pltpu
from jax.sharding import PartitionSpec as P

LN2 = math.log(2.0)
SCALE = 5.0 / (LN2 * LN2)
MESH = pl.DeviceIdType.MESH
TAIL = 16


def rounded(x):
    return x.astype(jnp.bfloat16).astype(jnp.float32)


def three_parts(x):
    high = rounded(x)
    rest = x - high
    middle = rounded(rest)
    return high, middle, rounded(rest - middle)


def matern(scaled_dist):
    dist = jnp.maximum(scaled_dist, 1e-30)
    root = dist * lax.rsqrt(dist)
    poly = 1.0 + root * (LN2 + (LN2 * LN2 / 3.0) * root)
    return (poly * jnp.exp2(-root)).astype(jnp.bfloat16)


def kernel(nb, nw, points_in, inv_in, noise_in, residual_in, direction_in, solution_in, solution_out, residual_out, direction_out,
           points, inv_length, direction, others, io, feat, feat_z, rows_x, cols_x, kmat, dir_a, dir_b, dir_rows, part_a, part_a_in, part_b, part_b_in, stat, stat_in,
           sent, feat_sem, feat_z_sem, dir_sem, got):
    b = lax.axis_index("blk")
    w = lax.axis_index("wide")
    chips = nb // 2
    chip, core = b // 2, b % 2
    features, piece = points.shape

    def other_chip(k):
        at, bit = chip, 1
        while bit < chips:
            if k & bit:
                at = at + bit - 2 * bit * lax.rem(lax.div(chip, bit), 2)
            bit *= 2
        return at

    def same_core(k):
        return (other_chip(k) * 2 + core, w)

    sibling = (chip * 2 + 1 - core, w)

    def along(q):
        return (b, lax.rem(w + q, nw))

    def at_least(limit):
        return lax.div(w + nw - limit, nw)

    upper = lax.div(2 * w, nw)

    def far_first(k):
        low = nw - 1 - k - at_least(nw - 1 - k)
        high = k + 1 - at_least(k + 1)
        return lax.rem(low + upper * (high - low) - w + nw, nw)

    z_far = [far_first(k) for k in range(nw - 1)]
    chips_far = sorted(range(1, chips), key=lambda k: -bin(k).count("1"))
    chips_near = chips_far[::-1]

    barrier = pltpu.get_barrier_semaphore()
    for k in range(1, chips):
        pl.semaphore_signal(barrier, inc=1, device_id=same_core(k), device_id_type=MESH)
    pl.semaphore_signal(barrier, inc=1, device_id=sibling, device_id_type=MESH)
    for q in range(1, nw):
        pl.semaphore_signal(barrier, inc=1, device_id=along(q), device_id_type=MESH)

    def copy(src, dst, send, recv, to):
        return pltpu.make_async_remote_copy(
            src_ref=src, dst_ref=dst, send_sem=send, recv_sem=recv, device_id=to, device_id_type=MESH
        )

    loads = [
        pltpu.make_async_copy(src, dst, io.at[min(k, 3)])
        for k, (src, dst) in enumerate(
            ((points_in, points), (inv_in, inv_length), (direction_in, direction),
             (residual_in, others.at[0]), (solution_in, others.at[1]))
        )
    ]
    for load in loads:
        load.start()
    for load in loads[:2]:
        load.wait()

    inv_row = jnp.concatenate(
        [inv_length[...], jnp.zeros((1, 128 - features), jnp.float32)], axis=1)
    inv_column = jnp.broadcast_to(inv_row, (8, 128)).T[:features, 0:1]
    x_t = rounded(points[...].astype(jnp.float32) * inv_column)
    feat[0] = x_t.astype(jnp.bfloat16)
    pl.semaphore_wait(barrier, chips + nw - 1)

    FEAT, FEAT_Z, DIR, DIR_Z, PART, PART_Z, STAT = range(7)

    def feat_copy(src_slot, dst_slot, to):
        return copy(feat.at[src_slot], feat.at[dst_slot], sent.at[FEAT], feat_sem.at[dst_slot - 1], to)

    def dir_copy(src_slot, dst_slot, to):
        return copy(dir_a.at[src_slot], dir_a.at[dst_slot], sent.at[DIR], dir_sem.at[min(dst_slot, chips) - 1], to)

    def feat_z_copy(src, slot, q):
        return copy(src, feat_z.at[slot], sent.at[FEAT_Z], feat_z_sem.at[slot - 1], along(q))

    for q in z_far:
        feat_z_copy(feat.at[0], nw - q, q).start()
    for k in chips_far:
        feat_copy(0, k, same_core(k)).start()
    feat_copy(0, chips, sibling).start()
    loads[2].wait()
    dir_t = direction[...].T.astype(jnp.bfloat16)
    part = dir_t.shape[0] // 2
    dir_a[0] = dir_t[:part]
    dir_b[0] = dir_t[part:]
    for k in chips_far:
        dir_copy(0, k, same_core(k)).start()
    dir_copy(0, chips, sibling).start()
    dir_rows[0:piece] = direction[...][:, :part].astype(jnp.bfloat16)

    def feat_arrived(slot):
        feat_copy(slot, slot, sibling).wait_recv()

    def relay_feat(k):
        feat_arrived(k)
        feat_copy(k, chips + k, sibling).start()

    def turn(slot):
        dir_rows[at_rows(slot), :] = dir_a[slot].astype(jnp.float32).T.astype(jnp.bfloat16)

    def relay_dir(k):
        dir_copy(k, k, sibling).wait_recv()
        dir_copy(k, chips + k, sibling).start()

    depth = rows_x.shape[1]
    ones = jnp.where(lax.broadcasted_iota(jnp.int32, (8, piece), 0) < 3, 1.0, 0.0)
    at = lax.broadcasted_iota(jnp.int32, (8, piece), 0)
    blank = jnp.zeros((depth - 3 * features - 16, piece), jnp.float32)

    def norms(x, first):
        result = jnp.zeros((8, piece), jnp.float32)
        for k, value in enumerate(three_parts(SCALE * jnp.sum(x * x, axis=0, keepdims=True))):
            result = jnp.where(at == first + k, value, result)
        return result

    def make_rows(j, block):
        x = block.astype(jnp.float32)
        lanes = jnp.concatenate(
            [-2.0 * value for value in three_parts(SCALE * x)] + [ones, norms(x, 0), blank], axis=0)
        rows_x[j * piece : (j + 1) * piece] = lanes.T.astype(jnp.bfloat16)

    def make_cols(slot):
        block = feat[slot]
        tail = jnp.concatenate([norms(block.astype(jnp.float32), 0), ones, blank], axis=0)
        cols_x[slot] = jnp.concatenate([block] * 3 + [tail.astype(jnp.bfloat16)], axis=0)

    start = lax.div(w, nw)

    def stored(j, count=1):
        return pl.ds(pl.multiple_of((start + j) * piece, piece), count * piece)

    def at_rows(j):
        return slice(j * piece, (j + 1) * piece)

    z_near = [0] + z_far[::-1]

    have_rows, have_cols, due = [], [], []

    def flush():
        for j, slot in due:
            dist = jnp.dot(rows_x[at_rows(j), :], cols_x[slot], preferred_element_type=jnp.float32)
            kmat[at_rows(j), at_rows(slot)] = matern(dist)
        due.clear()

    def add_rows(j):
        if j:
            q = z_near[j]
            feat_z_copy(feat_z.at[q], q, q).wait_recv()
            make_rows(j, feat_z[q])
        else:
            make_rows(0, feat[0])
        flush()
        due.extend((j, slot) for slot in have_cols)
        have_rows.append(j)

    def add_cols(slot):
        if slot >= chips:
            feat_arrived(slot)
        make_cols(slot)
        flush()
        due.extend((j, slot) for j in have_rows)
        have_cols.append(slot)

    every = range(nw)
    near, last = chips_near[:-1], chips_near[-1:]
    add_rows(0)
    add_cols(0)
    add_cols(chips)
    flush()
    for q in z_far:
        copy(dir_b.at[0], dir_b.at[nw - q], sent.at[DIR_Z], got.at[DIR_Z], along(q)).start()
    for k in near:
        relay_feat(k)
    for k in near:
        add_cols(k)
    if nw > 1:
        add_rows(1)
    for k in last:
        relay_feat(k)
        add_cols(k)
    for k in near:
        add_cols(chips + k)
    for j in range(2, nw - 1):
        add_rows(j)
    for k in near:
        relay_dir(k)
    for j in range(max(2, nw - 1), nw):
        add_rows(j)
    for k in last:
        relay_dir(k)
    for k in last:
        add_cols(chips + k)
    for k in range(1, chips):
        turn(k)
    flush()

    def product_a(rows):
        product = jnp.dot(kmat[stored(rows[0], len(rows)), :], dir_rows[...], preferred_element_type=jnp.float32)
        return {j: product[at * piece : (at + 1) * piece].T for at, j in enumerate(rows)}

    def product_b(slot):
        total = None
        for j in every:
            term = jnp.dot(dir_b[z_near[j]], kmat[stored(j), at_rows(slot)],
                           preferred_element_type=jnp.float32)
            total = term if total is None else total + term
        return total

    def send_a(j, value):
        q = z_near[j]
        part_a[j] = value.astype(jnp.bfloat16)
        copy(part_a.at[j], part_a_in.at[nw - q], sent.at[PART_Z], got.at[PART_Z], along(q)).start()

    def send_b(k, c, value):
        slot = c * chips + k
        to = (other_chip(k) * 2 + (1 - core if c else core), w)
        part_b[slot] = value.astype(jnp.bfloat16)
        copy(part_b.at[slot], part_b_in.at[slot], sent.at[PART], got.at[PART], to).start()

    def all_of(ref, kind, recv):
        return copy(ref, ref, sent.at[kind], recv, sibling)

    relayed, z_dirs = dir_a.at[pl.ds(chips, chips)], dir_b.at[pl.ds(1, nw - 1)]
    all_of(relayed, DIR, dir_sem.at[chips - 1]).wait_recv()
    for k in range(chips):
        turn(chips + k)
    all_of(z_dirs, DIR_Z, got.at[DIR_Z]).wait_recv()
    total_a = total_b = None
    for step in range(max(nw, chips)):
        j = nw - 1 - step
        k = (chips_far + [0])[step] if step < chips else None
        if j >= 0:
            a = product_a([j])[j]
        if k is not None:
            both = [product_b(k), product_b(chips + k)]
        if j > 0:
            send_a(j, a)
        elif j == 0:
            total_a = a
        if k:
            send_b(k, 0, both[0])
        elif k == 0:
            total_b = both[0]
        if k is not None:
            send_b(k, 1, both[1])
    parts_z, parts_b = part_a_in.at[pl.ds(1, nw - 1)], part_b_in.at[pl.ds(1, nb - 1)]
    all_of(parts_z, PART_Z, got.at[PART_Z]).wait_recv()
    for q in range(1, nw):
        total_a = total_a + part_a_in[q].astype(jnp.float32)
    all_of(parts_b, PART, got.at[PART]).wait_recv()
    for slot in range(1, nb):
        total_b = total_b + part_b_in[slot].astype(jnp.float32)
    make_vectors = pltpu.make_async_copy(others, others, io.at[3])
    make_vectors.wait()
    res, direc = others[0], direction[...]
    total = jnp.concatenate([total_a, total_b], axis=0).T + noise_in[0, 0] * direc

    for k, value in enumerate((res * res, direc * total, res * total, total * total)):
        stat[k : k + 1] = jnp.sum(value, axis=0, keepdims=True)
    for r, q in enumerate(z_far + [0]):
        for k in chips_far + [0]:
            for c in range(2):
                if r == nw - 1 and k == 0 and c == 0:
                    continue
                to = (other_chip(k) * 2 + (core if c == 0 else 1 - core), lax.rem(w + q, nw))
                slot = (lax.rem(nw - q, nw) * 2 + c) * chips + k
                copy(stat, stat_in.at[slot], sent.at[STAT], got.at[STAT], to).start()
    stats = stat_in.at[pl.ds(1, nb * nw - 1)]
    all_of(stats, STAT, got.at[STAT]).wait_recv()
    sums = stat[...]
    for slot in range(1, nb * nw):
        sums = sums + stat_in[slot]
    old_norm, step = sums[0:1], sums[0:1] / sums[1:2]
    new_norm = old_norm - 2.0 * step * sums[2:3] + step * step * sums[3:4]
    new_residual = res - step * total
    residual_out[...] = new_residual
    solution_out[...] = others[1] + step * direc
    direction_out[...] = new_residual + new_norm / old_norm * direc
    for ref, kind in ((feat.at[pl.ds(1, nb - 1)], FEAT), (feat_z.at[pl.ds(1, nw - 1)], FEAT_Z), (dir_a.at[pl.ds(1, nb - 1)], DIR),
                      (z_dirs, DIR_Z), (parts_b, PART), (parts_z, PART_Z), (stats, STAT)):
        all_of(ref, kind, got.at[kind]).wait_send()


def long_kernel(nb, nw, points_in, inv_in, noise_in, residual_in, direction_in, solution_in, solution_out, residual_out, direction_out,
           points, inv_length, noise_var, residual, direction, old_solution, io, feat, feat_z, rows_x, kmat, low_dir, part, part_in, stat, stat_z, stat_b, stat_o,
           fs, fr, fzs, fzr, ps, pr, qs, qr, zs, zr, bs, br):
    b = lax.axis_index("blk")
    w = lax.axis_index("wide")
    chips = nb // 2
    chip, core = b // 2, b % 2
    features, piece = points.shape

    def same_core(q):
        return (lax.rem(chip + q, chips) * 2 + core, w)

    sibling = (chip * 2 + 1 - core, w)

    def along(q):
        return (b, lax.rem(w + q, nw))

    def plane(slot):
        return (lax.rem(chip + slot // 2, chips) * 2 + (core if slot % 2 == 0 else 1 - core), w)

    def back(slot):
        return (chips - slot // 2) % chips * 2 + slot % 2

    barrier = pltpu.get_barrier_semaphore()
    for slot in range(1, nb):
        pl.semaphore_signal(barrier, inc=1, device_id=plane(slot), device_id_type=MESH)
    for q in range(1, nw):
        pl.semaphore_signal(barrier, inc=1, device_id=along(q), device_id_type=MESH)

    def copy(src, dst, send, recv, to):
        return pltpu.make_async_remote_copy(
            src_ref=src, dst_ref=dst, send_sem=send, recv_sem=recv, device_id=to, device_id_type=MESH
        )

    loads = [
        pltpu.make_async_copy(src, dst, io.at[k])
        for k, (src, dst) in enumerate(
            ((points_in, points), (inv_in, inv_length), (direction_in, direction),
             (residual_in, residual), (solution_in, old_solution))
        )
    ]
    for load in loads:
        load.start()
    for load in loads[:2]:
        load.wait()

    inv_row = jnp.concatenate(
        [inv_length[...], jnp.zeros((1, 128 - features), jnp.float32)], axis=1)
    inv_column = jnp.broadcast_to(inv_row, (8, 128)).T[:features, 0:1]
    x_t = rounded(points[...].astype(jnp.float32) * inv_column)
    s1, s2, s3 = three_parts(SCALE * jnp.sum(x_t * x_t, axis=0, keepdims=True))
    row = lax.broadcasted_iota(jnp.int32, (TAIL, piece), 0)
    tail = jnp.where((row >= 3) & (row <= 10), 1.0, 0.0)
    tail = jnp.where((row >= 6) & (row <= 7), 0.0, tail)
    for at, value in ((0, s1), (1, s2), (2, s3), (11, s1), (12, s2), (13, s3)):
        tail = jnp.where(row == at, value, tail)
    feat[0] = jnp.concatenate([x_t, tail], axis=0).astype(jnp.bfloat16)
    for load in loads[2:]:
        load.wait()
    low_dir[0:piece] = direction[...].astype(jnp.bfloat16)
    pl.semaphore_wait(barrier, nb - 1 + nw - 1)

    upper = lax.div(2 * w, nw)

    def near(k):
        return k + upper * (nw - 2 * k)

    def rows_at(q):
        return pl.ds(pl.multiple_of(q * piece, piece), piece)

    sends = []

    def go(c):
        c.start()
        sends.append(c)
        return c

    def feat_copy(src_slot, dst_slot, to):
        return copy(feat.at[src_slot], feat.at[dst_slot], fs.at[dst_slot], fr.at[dst_slot], to)

    def dir_copy(src_slot, dst_slot, to):
        return copy(low_dir.at[pl.ds(src_slot * piece, piece)], low_dir.at[pl.ds(dst_slot * piece, piece)],
                    ps.at[dst_slot], pr.at[dst_slot], to)

    for k in range(1, nw):
        q = near(nw - k)
        go(copy(feat.at[0], feat_z.at[nw - q], fzs.at[q], fzr.at[nw - q], along(q)))
    go(feat_copy(0, 1, sibling))
    for q in range(1, chips):
        go(feat_copy(0, 2 * (chips - q), same_core(q)))
    for q in range(1, chips):
        go(dir_copy(0, 2 * (chips - q), same_core(q)))
    go(dir_copy(0, 1, sibling))

    def feat_arrived(slot):
        feat_copy(slot, slot, sibling).wait_recv()

    def dir_arrived(slot):
        dir_copy(slot, slot, sibling).wait_recv()

    def as_rows(block):
        block = block.astype(jnp.float32)
        x = block[:features]
        h, m, l = three_parts(SCALE * x)
        lanes = jnp.concatenate(
            [-2.0 * h, -2.0 * m, -2.0 * l, block[features + 8 :],
             jnp.zeros((TAIL + 8, piece), jnp.float32)], axis=0)
        return lanes.T.astype(jnp.bfloat16)

    depth = rows_x.shape[1]

    def tile(at, slot):
        block = feat[slot]
        cols = jnp.concatenate(
            [block[:features]] * 3 + [block[features:],
             jnp.zeros((depth - 3 * features - TAIL, piece), jnp.bfloat16)], axis=0)
        dist = jnp.dot(rows_x[at, :], cols, preferred_element_type=jnp.float32)
        kmat[at, slot * piece : (slot + 1) * piece] = matern(dist)

    def feat_z_arrived(q):
        copy(feat_z.at[q], feat_z.at[q], fzs.at[q], fzr.at[q], along(q)).wait_recv()

    def relay_direction(q):
        dir_arrived(2 * q)
        go(dir_copy(2 * q, 2 * q + 1, sibling))

    rows_x[0:piece] = as_rows(feat[0])
    tile(pl.ds(0, piece), 0)
    feat_arrived(1)
    tile(pl.ds(0, piece), 1)
    for q in range(1, chips):
        feat_arrived(2 * q)
        go(feat_copy(2 * q, 2 * q + 1, sibling))
        tile(pl.ds(0, piece), 2 * q)
    for q in range(1, chips):
        feat_arrived(2 * q + 1)
        tile(pl.ds(0, piece), 2 * q + 1)
    if nw <= 4:
        relayed = 1
        for k in range(1, nw):
            q = near(k)
            feat_z_arrived(q)
            rows_x[rows_at(q), :] = as_rows(feat_z[q])
            for slot in range(nb):
                tile(rows_at(q), slot)
                if k == nw - 1 and slot in (0, nb // 2) and relayed < chips:
                    relay_direction(relayed)
                    relayed += 1
    else:
        relayed = 1
        for q in range(1, nw):
            feat_z_arrived(q)
            rows_x[q * piece : (q + 1) * piece] = as_rows(feat_z[q])

        def row_tiles(q, carry):
            for slot in range(nb):
                tile(pl.ds(pl.multiple_of(q * piece, piece), piece), slot)
            return carry

        lax.fori_loop(1, nw, row_tiles, 0)
    for q in range(relayed, chips):
        relay_direction(q)
    for q in range(chips):
        dir_arrived(2 * q + 1)

    def partial(q):
        return jnp.dot(kmat[rows_at(q), :], low_dir[...],
                       preferred_element_type=jnp.float32)

    for k in range(1, nw):
        q = near(nw - k)
        part[q] = partial(q).astype(jnp.bfloat16)
        go(copy(part.at[q], part_in.at[nw - q], qs.at[q], qr.at[nw - q], along(q)))
    total = partial(0) + noise_in[0, 0] * direction[...]
    for q in range(1, nw):
        copy(part.at[q], part_in.at[q], qs.at[q], qr.at[q], along(q)).wait_recv()
        total = total + part_in[q].astype(jnp.float32)

    def column_sum(x):
        return jnp.sum(x, axis=0, keepdims=True)

    res, direc = residual[...], direction[...]
    at = lax.broadcasted_iota(jnp.int32, (8, res.shape[1]), 0)
    sums = jnp.zeros(at.shape, jnp.float32)
    for k, value in enumerate((res * res, direc * total, res * total, total * total)):
        sums = jnp.where(at == k, column_sum(value), sums)
    stat[...] = sums
    for q in range(1, nw):
        go(copy(stat, stat_z.at[nw - q], zs.at[q], zr.at[nw - q], along(q)))
    for q in range(1, nw):
        copy(stat, stat_z.at[q], zs.at[q], zr.at[q], along(q)).wait_recv()
        sums = sums + stat_z[q]
    stat_o[...] = sums
    for slot in range(1, nb):
        go(copy(stat_o, stat_b.at[back(slot)], bs.at[slot], br.at[back(slot)], plane(slot)))
    for slot in range(1, nb):
        copy(stat_o, stat_b.at[slot], bs.at[slot], br.at[slot], plane(slot)).wait_recv()
        sums = sums + stat_b[slot]
    old_norm, step = sums[0:1], sums[0:1] / sums[1:2]
    new_norm = old_norm - 2.0 * step * sums[2:3] + step * step * sums[3:4]
    new_residual = res - step * total
    residual_out[...] = new_residual
    solution_out[...] = old_solution[...] + step * direc
    direction_out[...] = new_residual + new_norm / old_norm * direc
    for c in sends:
        c.wait_send()


def write_out(a, b, c, a_out, b_out, c_out, sems):
    copies = [
        pltpu.make_async_copy(src, dst, sems.at[k])
        for k, (src, dst) in enumerate(((a, a_out), (b, b_out), (c, c_out)))
    ]
    for copy in copies:
        copy.start()
    for copy in copies:
        copy.wait()


def on_device(nb, nw, points, inv_length, noise_var, solution, residual, direction):
    piece, features = points.shape
    rhs = direction.shape[1]
    vmem = pl.BlockSpec(memory_space=pltpu.VMEM)
    hbm = pl.BlockSpec(memory_space=pl.ANY)
    dma = pltpu.SemaphoreType.DMA
    depth = 3 * features + 2 * TAIL
    common = [
        pltpu.VMEM((features, piece), points.dtype),
        pltpu.VMEM((1, features), jnp.float32),
    ]
    wide = [
        dma((6,)),
        pltpu.VMEM((nb, features + TAIL, piece), jnp.bfloat16),
        pltpu.VMEM((nw, features + TAIL, piece), jnp.bfloat16),
        pltpu.VMEM((nw * piece, depth), jnp.bfloat16),
        pltpu.VMEM((nw * piece, nb * piece), jnp.bfloat16),
        pltpu.VMEM((nb * piece, rhs), jnp.bfloat16),
    ]
    vectors = [pltpu.VMEM((piece, rhs), jnp.float32)] * 3
    parts = [pltpu.VMEM((nw, piece, rhs), jnp.bfloat16)] * 2
    sems = [dma((nb,)), dma((nb,)), dma((nw,)), dma((nw,)), dma((nb,)), dma((nb,)), dma((nw,)), dma((nw,))]
    if nw <= 4:
        body = kernel
        half = rhs // 2
        low = jnp.bfloat16
        scratch = common + [
            pltpu.VMEM((piece, rhs), jnp.float32), pltpu.VMEM((2, piece, rhs), jnp.float32), dma((4,)),
            pltpu.VMEM((nb, features, piece), low), pltpu.VMEM((nw, features, piece), low),
            pltpu.VMEM((nw * piece, depth), low), pltpu.VMEM((nb, depth, piece), low),
            pltpu.VMEM((nw * piece, nb * piece), low),
            pltpu.VMEM((nb, half, piece), low), pltpu.VMEM((nw, half, piece), low),
            pltpu.VMEM((nb * piece, half), low),
            pltpu.VMEM((nw, half, piece), low), pltpu.VMEM((nw, half, piece), low),
            pltpu.VMEM((nb, half, piece), low), pltpu.VMEM((nb, half, piece), low),
            pltpu.VMEM((4, rhs), jnp.float32), pltpu.VMEM((nw * nb, 4, rhs), jnp.float32),
            dma((7,)), dma((nb - 1,)), dma((nw - 1,)), dma((nb // 2,)), dma((7,)),
        ]
    else:
        body = long_kernel
        scratch = common + [pltpu.VMEM((1, 1), jnp.float32)] + vectors + wide + parts + [
            pltpu.VMEM((8, rhs), jnp.float32),
            pltpu.VMEM((nw, 8, rhs), jnp.float32),
            pltpu.VMEM((nb, 8, rhs), jnp.float32),
            pltpu.VMEM((8, rhs), jnp.float32),
        ] + sems + [dma((nw,)), dma((nw,)), dma((nb,)), dma((nb,))]
    news = pl.pallas_call(
        functools.partial(body, nb, nw),
        out_shape=(pltpu.VMEM((piece, rhs), jnp.float32),) * 3,
        in_specs=[hbm, hbm, pl.BlockSpec(memory_space=pltpu.SMEM), hbm, hbm, hbm],
        out_specs=(vmem,) * 3,
        scratch_shapes=scratch,
        compiler_params=pltpu.CompilerParams(
            collective_id=0, has_side_effects=True, vmem_limit_bytes=60 * 1024 * 1024
        ),
    )(points.T, inv_length.reshape(1, features), noise_var.reshape(1, 1), residual, direction, solution)
    return pl.pallas_call(
        write_out,
        out_shape=(jax.ShapeDtypeStruct((piece, rhs), jnp.float32),) * 3,
        in_specs=[vmem] * 3,
        out_specs=(hbm,) * 3,
        scratch_shapes=[dma((3,))],
    )(*(pltpu.with_memory_space_constraint(x, pltpu.VMEM) for x in news))


def solution(mesh):
    spec = P(("blk", "wide"), None)
    return jax.shard_map(
        functools.partial(on_device, mesh.shape["blk"], mesh.shape["wide"]),
        mesh=mesh,
        in_specs=(spec, P(), P(), spec, spec, spec),
        out_specs=(spec, spec, spec),
        check_vma=False,
    )
```

```python
import functools
import math

import jax
import jax.numpy as jnp
from jax import lax
from jax.experimental import pallas as pl
from jax.experimental.pallas import tpu as pltpu
from jax.sharding import PartitionSpec as P

ROOT3 = math.sqrt(3.0)
SCALE = 5.0 / 3.0
MESH = pl.DeviceIdType.MESH
TAIL = 16


def rounded(x):
    return x.astype(jnp.bfloat16).astype(jnp.float32)


def three_parts(x):
    high = rounded(x)
    rest = x - high
    middle = rounded(rest)
    return high, middle, rounded(rest - middle)


def matern(scaled_dist):
    dist = jnp.maximum(scaled_dist, 1e-30)
    root = dist * lax.rsqrt(dist)
    poly = root * (root + ROOT3) + 1.0
    return (poly * jnp.exp2(root * (-ROOT3 / math.log(2.0)))).astype(jnp.bfloat16)


def kernel(nb, nw, points_in, inv_in, noise_in, residual_in, direction_in, solution_in, solution_out, residual_out, direction_out,
           points, inv_length, direction, others, io, feat, feat_z, rows_x, cols_x, kmat, dir_a, dir_b, dir_rows, part_a, part_a_in, part_b, part_b_in, stat, stat_in,
           sent, feat_sem, feat_z_sem, dir_sem, got):
    b = lax.axis_index("blk")
    w = lax.axis_index("wide")
    chips = nb // 2
    chip, core = b // 2, b % 2
    features, piece = points.shape

    def other_chip(k):
        at, bit = chip, 1
        while bit < chips:
            if k & bit:
                at = at + bit - 2 * bit * lax.rem(lax.div(chip, bit), 2)
            bit *= 2
        return at

    def same_core(k):
        return (other_chip(k) * 2 + core, w)

    sibling = (chip * 2 + 1 - core, w)

    def along(q):
        return (b, lax.rem(w + q, nw))

    def at_least(limit):
        return lax.div(w + nw - limit, nw)

    upper = lax.div(2 * w, nw)

    def far_first(k):
        low = nw - 1 - k - at_least(nw - 1 - k)
        high = k + 1 - at_least(k + 1)
        return lax.rem(low + upper * (high - low) - w + nw, nw)

    z_far = [far_first(k) for k in range(nw - 1)]
    chips_far = sorted(range(1, chips), key=lambda k: -bin(k).count("1"))
    chips_near = chips_far[::-1]

    def copy(src, dst, send, recv, to):
        return pltpu.make_async_remote_copy(
            src_ref=src, dst_ref=dst, send_sem=send, recv_sem=recv, device_id=to, device_id_type=MESH
        )

    loads = [
        pltpu.make_async_copy(src, dst, io.at[min(k, 3)])
        for k, (src, dst) in enumerate(
            ((points_in, points), (inv_in, inv_length), (direction_in, direction),
             (residual_in, others.at[0]), (solution_in, others.at[1]))
        )
    ]
    for load in loads[:2]:
        load.start()
    barrier = pltpu.get_barrier_semaphore()
    for q in z_far:
        pl.semaphore_signal(barrier, inc=1, device_id=along(q), device_id_type=MESH)
    for k in chips_far:
        pl.semaphore_signal(barrier, inc=1, device_id=same_core(k), device_id_type=MESH)
    pl.semaphore_signal(barrier, inc=1, device_id=sibling, device_id_type=MESH)
    for load in loads[2:]:
        load.start()
    for load in loads[:2]:
        load.wait()

    inv_row = jnp.concatenate(
        [inv_length[...], jnp.zeros((1, 128 - features), jnp.float32)], axis=1)
    inv_column = jnp.broadcast_to(inv_row, (8, 128)).T[:features, 0:1]
    x_t = rounded(points[...].astype(jnp.float32) * inv_column)
    feat[0] = x_t.astype(jnp.bfloat16)
    pl.semaphore_wait(barrier, chips + nw - 1)

    DIR_Z, PART, PART_Z, STAT, FEAT, FEAT_Z, DIR = range(7)

    def feat_copy(src_slot, dst_slot, to):
        return copy(feat.at[src_slot], feat.at[dst_slot], sent.at[FEAT], feat_sem.at[dst_slot - 1], to)

    def dir_copy(src_slot, dst_slot, to):
        return copy(dir_a.at[src_slot], dir_a.at[dst_slot], sent.at[DIR], dir_sem.at[min(dst_slot, chips) - 1], to)

    def feat_z_copy(src, slot, q):
        return copy(src, feat_z.at[slot], sent.at[FEAT_Z], feat_z_sem.at[slot - 1], along(q))

    for q in z_far:
        feat_z_copy(feat.at[0], nw - q, q).start()
    feat_copy(0, chips, sibling).start()
    for k in chips_near:
        feat_copy(0, k, same_core(k)).start()
    loads[2].wait()
    dir_t = direction[...].T.astype(jnp.bfloat16)
    part = dir_t.shape[0] // 2
    dir_a[0] = dir_t[:part]
    dir_b[0] = dir_t[part:]
    for k in chips_far:
        dir_copy(0, k, same_core(k)).start()
    dir_copy(0, chips, sibling).start()
    dir_rows[0:piece] = direction[...][:, :part].astype(jnp.bfloat16)

    def feat_arrived(slot):
        feat_copy(slot, slot, sibling).wait_recv()

    def relay_feat(k):
        feat_arrived(k)
        feat_copy(k, chips + k, sibling).start()

    def turn(slot):
        dir_rows[at_rows(slot), :] = dir_a[slot].astype(jnp.float32).T.astype(jnp.bfloat16)

    def relay_dir(k):
        dir_copy(k, k, sibling).wait_recv()
        dir_copy(k, chips + k, sibling).start()

    depth = rows_x.shape[1]
    ones = jnp.where(lax.broadcasted_iota(jnp.int32, (8, piece), 0) < 3, 1.0, 0.0)
    at = lax.broadcasted_iota(jnp.int32, (8, piece), 0)
    blank = jnp.zeros((depth - 3 * features - 16, piece), jnp.float32)

    def norms(x, first):
        result = jnp.zeros((8, piece), jnp.float32)
        for k, value in enumerate(three_parts(SCALE * jnp.sum(x * x, axis=0, keepdims=True))):
            result = jnp.where(at == first + k, value, result)
        return result

    def make_rows(j, block):
        x = block.astype(jnp.float32)
        lanes = jnp.concatenate(
            [-2.0 * value for value in three_parts(SCALE * x)] + [ones, norms(x, 0), blank], axis=0)
        rows_x[j * piece : (j + 1) * piece] = lanes.T.astype(jnp.bfloat16)

    def make_cols(slot):
        block = feat[slot]
        tail = jnp.concatenate([norms(block.astype(jnp.float32), 0), ones, blank], axis=0)
        cols_x[slot] = jnp.concatenate([block] * 3 + [tail.astype(jnp.bfloat16)], axis=0)

    start = lax.div(w, nw)

    def stored(j, count=1):
        return pl.ds(pl.multiple_of((start + j) * piece, piece), count * piece)

    def at_rows(j):
        return slice(j * piece, (j + 1) * piece)

    z_near = [0] + z_far[::-1]

    have_rows, have_cols, due = [], [], []

    def flush():
        for j, slot in due:
            dist = jnp.dot(rows_x[at_rows(j), :], cols_x[slot], preferred_element_type=jnp.float32)
            kmat[at_rows(j), at_rows(slot)] = matern(dist)
        due.clear()

    def add_rows(j):
        if j:
            q = z_near[j]
            feat_z_copy(feat_z.at[q], q, q).wait_recv()
            make_rows(j, feat_z[q])
        else:
            make_rows(0, feat[0])
        flush()
        due.extend((j, slot) for slot in have_cols)
        have_rows.append(j)

    def add_cols(slot):
        if slot >= chips:
            feat_arrived(slot)
        make_cols(slot)
        flush()
        due.extend((j, slot) for j in have_rows)
        have_cols.append(slot)

    every = range(nw)
    near, last = chips_near[:-1], chips_near[-1:]
    add_rows(0)
    add_cols(0)
    add_cols(chips)
    flush()
    for q in z_far:
        copy(dir_b.at[0], dir_b.at[nw - q], sent.at[DIR_Z], got.at[DIR_Z], along(q)).start()
    for k in near:
        relay_feat(k)
    for k in near:
        add_cols(k)
    if nw > 1:
        add_rows(1)
    for k in last:
        relay_feat(k)
        add_cols(k)
    for k in near:
        add_cols(chips + k)
    for k in near:
        relay_dir(k)
    for j in range(2, nw - 1):
        add_rows(j)
    for k in last:
        relay_dir(k)
    for j in range(max(2, nw - 1), nw):
        add_rows(j)
    for k in last:
        add_cols(chips + k)
    for k in range(1, chips):
        turn(k)
    flush()

    def product_a(rows):
        product = jnp.dot(kmat[stored(rows[0], len(rows)), :], dir_rows[...], preferred_element_type=jnp.float32)
        return {j: product[at * piece : (at + 1) * piece].T for at, j in enumerate(rows)}

    def product_b(slot):
        total = None
        for j in every:
            term = jnp.dot(dir_b[z_near[j]], kmat[stored(j), at_rows(slot)],
                           preferred_element_type=jnp.float32)
            total = term if total is None else total + term
        return total

    def send_a(j, value):
        q = z_near[j]
        part_a[j] = value.astype(jnp.bfloat16)
        copy(part_a.at[j], part_a_in.at[nw - q], sent.at[PART_Z], got.at[PART_Z], along(q)).start()

    def send_b(k, c, value):
        slot = c * chips + k
        to = (other_chip(k) * 2 + (1 - core if c else core), w)
        part_b[slot] = value.astype(jnp.bfloat16)
        copy(part_b.at[slot], part_b_in.at[slot], sent.at[PART], got.at[PART], to).start()

    def all_of(ref, kind, recv):
        return copy(ref, ref, sent.at[kind], recv, sibling)

    relayed, z_dirs = dir_a.at[pl.ds(chips, chips)], dir_b.at[pl.ds(1, nw - 1)]
    all_of(relayed, DIR, dir_sem.at[chips - 1]).wait_recv()
    for k in range(chips):
        turn(chips + k)
    all_of(z_dirs, DIR_Z, got.at[DIR_Z]).wait_recv()
    total_a = total_b = None
    for step in range(max(nw, chips)):
        j = nw - 1 - step
        k = (chips_far + [0])[step] if step < chips else None
        if j >= 0:
            a = product_a([j])[j]
        if k is not None:
            both = [product_b(k), product_b(chips + k)]
        if j > 0:
            send_a(j, a)
        elif j == 0:
            total_a = a
        if k:
            send_b(k, 0, both[0])
        elif k == 0:
            total_b = both[0]
        if k is not None:
            send_b(k, 1, both[1])
    parts_z, parts_b = part_a_in.at[pl.ds(1, nw - 1)], part_b_in.at[pl.ds(1, nb - 1)]
    all_of(parts_z, PART_Z, got.at[PART_Z]).wait_recv()
    for q in range(1, nw):
        total_a = total_a + part_a_in[q].astype(jnp.float32)
    all_of(parts_b, PART, got.at[PART]).wait_recv()
    for slot in range(1, nb):
        total_b = total_b + part_b_in[slot].astype(jnp.float32)
    make_vectors = pltpu.make_async_copy(others, others, io.at[3])
    make_vectors.wait()
    res, direc = others[0], direction[...]
    total = jnp.concatenate([total_a, total_b], axis=0).T + noise_in[0, 0] * direc

    for k, value in enumerate((res * res, direc * total, res * total, total * total)):
        stat[k : k + 1] = jnp.sum(value, axis=0, keepdims=True)
    for r, q in enumerate(z_far + [0]):
        for k in chips_far + [0]:
            for c in range(2):
                if r == nw - 1 and k == 0 and c == 0:
                    continue
                to = (other_chip(k) * 2 + (core if c == 0 else 1 - core), lax.rem(w + q, nw))
                slot = (lax.rem(nw - q, nw) * 2 + c) * chips + k
                copy(stat, stat_in.at[slot], sent.at[STAT], got.at[STAT], to).start()
    stats = stat_in.at[pl.ds(1, nb * nw - 1)]
    all_of(stats, STAT, got.at[STAT]).wait_recv()
    sums = stat[...]
    for slot in range(1, nb * nw):
        sums = sums + stat_in[slot]
    old_norm, step = sums[0:1], sums[0:1] / sums[1:2]
    new_norm = old_norm - 2.0 * step * sums[2:3] + step * step * sums[3:4]
    new_residual = res - step * total
    residual_out[...] = new_residual
    solution_out[...] = others[1] + step * direc
    direction_out[...] = new_residual + new_norm / old_norm * direc
    for ref, kind in ((feat.at[pl.ds(1, nb - 1)], FEAT), (feat_z.at[pl.ds(1, nw - 1)], FEAT_Z), (dir_a.at[pl.ds(1, nb - 1)], DIR),
                      (z_dirs, DIR_Z), (parts_b, PART), (parts_z, PART_Z), (stats, STAT)):
        all_of(ref, kind, got.at[STAT]).wait_send()


def long_kernel(nb, nw, points_in, inv_in, noise_in, residual_in, direction_in, solution_in, solution_out, residual_out, direction_out,
           points, inv_length, noise_var, residual, direction, old_solution, io, feat, feat_z, rows_x, kmat, low_dir, part, part_in, stat, stat_z, stat_b, stat_o,
           fs, fr, fzs, fzr, ps, pr, qs, qr, zs, zr, bs, br):
    b = lax.axis_index("blk")
    w = lax.axis_index("wide")
    chips = nb // 2
    chip, core = b // 2, b % 2
    features, piece = points.shape

    def same_core(q):
        return (lax.rem(chip + q, chips) * 2 + core, w)

    sibling = (chip * 2 + 1 - core, w)

    def along(q):
        return (b, lax.rem(w + q, nw))

    def plane(slot):
        return (lax.rem(chip + slot // 2, chips) * 2 + (core if slot % 2 == 0 else 1 - core), w)

    def back(slot):
        return (chips - slot // 2) % chips * 2 + slot % 2

    barrier = pltpu.get_barrier_semaphore()
    for slot in range(1, nb):
        pl.semaphore_signal(barrier, inc=1, device_id=plane(slot), device_id_type=MESH)
    for q in range(1, nw):
        pl.semaphore_signal(barrier, inc=1, device_id=along(q), device_id_type=MESH)

    def copy(src, dst, send, recv, to):
        return pltpu.make_async_remote_copy(
            src_ref=src, dst_ref=dst, send_sem=send, recv_sem=recv, device_id=to, device_id_type=MESH
        )

    loads = [
        pltpu.make_async_copy(src, dst, io.at[k])
        for k, (src, dst) in enumerate(
            ((points_in, points), (inv_in, inv_length), (direction_in, direction),
             (residual_in, residual), (solution_in, old_solution))
        )
    ]
    for load in loads:
        load.start()
    for load in loads[:2]:
        load.wait()

    inv_row = jnp.concatenate(
        [inv_length[...], jnp.zeros((1, 128 - features), jnp.float32)], axis=1)
    inv_column = jnp.broadcast_to(inv_row, (8, 128)).T[:features, 0:1]
    x_t = rounded(points[...].astype(jnp.float32) * inv_column)
    s1, s2, s3 = three_parts(SCALE * jnp.sum(x_t * x_t, axis=0, keepdims=True))
    row = lax.broadcasted_iota(jnp.int32, (TAIL, piece), 0)
    tail = jnp.where((row >= 3) & (row <= 10), 1.0, 0.0)
    tail = jnp.where((row >= 6) & (row <= 7), 0.0, tail)
    for at, value in ((0, s1), (1, s2), (2, s3), (11, s1), (12, s2), (13, s3)):
        tail = jnp.where(row == at, value, tail)
    feat[0] = jnp.concatenate([x_t, tail], axis=0).astype(jnp.bfloat16)
    for load in loads[2:]:
        load.wait()
    low_dir[0:piece] = direction[...].astype(jnp.bfloat16)
    pl.semaphore_wait(barrier, nb - 1 + nw - 1)

    upper = lax.div(2 * w, nw)

    def near(k):
        return k + upper * (nw - 2 * k)

    def rows_at(q):
        return pl.ds(pl.multiple_of(q * piece, piece), piece)

    sends = []

    def go(c):
        c.start()
        sends.append(c)
        return c

    def feat_copy(src_slot, dst_slot, to):
        return copy(feat.at[src_slot], feat.at[dst_slot], fs.at[dst_slot], fr.at[dst_slot], to)

    def dir_copy(src_slot, dst_slot, to):
        return copy(low_dir.at[pl.ds(src_slot * piece, piece)], low_dir.at[pl.ds(dst_slot * piece, piece)],
                    ps.at[dst_slot], pr.at[dst_slot], to)

    for k in range(1, nw):
        q = near(nw - k)
        go(copy(feat.at[0], feat_z.at[nw - q], fzs.at[q], fzr.at[nw - q], along(q)))
    go(feat_copy(0, 1, sibling))
    for q in range(1, chips):
        go(feat_copy(0, 2 * (chips - q), same_core(q)))
    for q in range(1, chips):
        go(dir_copy(0, 2 * (chips - q), same_core(q)))
    go(dir_copy(0, 1, sibling))

    def feat_arrived(slot):
        feat_copy(slot, slot, sibling).wait_recv()

    def dir_arrived(slot):
        dir_copy(slot, slot, sibling).wait_recv()

    def as_rows(block):
        block = block.astype(jnp.float32)
        x = block[:features]
        h, m, l = three_parts(SCALE * x)
        lanes = jnp.concatenate(
            [-2.0 * h, -2.0 * m, -2.0 * l, block[features + 8 :],
             jnp.zeros((TAIL + 8, piece), jnp.float32)], axis=0)
        return lanes.T.astype(jnp.bfloat16)

    depth = rows_x.shape[1]

    def tile(at, slot):
        block = feat[slot]
        cols = jnp.concatenate(
            [block[:features]] * 3 + [block[features:],
             jnp.zeros((depth - 3 * features - TAIL, piece), jnp.bfloat16)], axis=0)
        dist = jnp.dot(rows_x[at, :], cols, preferred_element_type=jnp.float32)
        kmat[at, slot * piece : (slot + 1) * piece] = matern(dist)

    def feat_z_arrived(q):
        copy(feat_z.at[q], feat_z.at[q], fzs.at[q], fzr.at[q], along(q)).wait_recv()

    def relay_direction(q):
        dir_arrived(2 * q)
        go(dir_copy(2 * q, 2 * q + 1, sibling))

    rows_x[0:piece] = as_rows(feat[0])
    tile(pl.ds(0, piece), 0)
    feat_arrived(1)
    tile(pl.ds(0, piece), 1)
    for q in range(1, chips):
        feat_arrived(2 * q)
        go(feat_copy(2 * q, 2 * q + 1, sibling))
        tile(pl.ds(0, piece), 2 * q)
    for q in range(1, chips):
        feat_arrived(2 * q + 1)
        tile(pl.ds(0, piece), 2 * q + 1)
    if nw <= 4:
        relayed = 1
        for k in range(1, nw):
            q = near(k)
            feat_z_arrived(q)
            rows_x[rows_at(q), :] = as_rows(feat_z[q])
            for slot in range(nb):
                tile(rows_at(q), slot)
                if k == nw - 1 and slot in (0, nb // 2) and relayed < chips:
                    relay_direction(relayed)
                    relayed += 1
    else:
        relayed = 1
        for q in range(1, nw):
            feat_z_arrived(q)
            rows_x[q * piece : (q + 1) * piece] = as_rows(feat_z[q])

        def row_tiles(q, carry):
            for slot in range(nb):
                tile(pl.ds(pl.multiple_of(q * piece, piece), piece), slot)
            return carry

        lax.fori_loop(1, nw, row_tiles, 0)
    for q in range(relayed, chips):
        relay_direction(q)
    for q in range(chips):
        dir_arrived(2 * q + 1)

    def partial(q):
        return jnp.dot(kmat[rows_at(q), :], low_dir[...],
                       preferred_element_type=jnp.float32)

    for k in range(1, nw):
        q = near(nw - k)
        part[q] = partial(q).astype(jnp.bfloat16)
        go(copy(part.at[q], part_in.at[nw - q], qs.at[q], qr.at[nw - q], along(q)))
    total = partial(0) + noise_in[0, 0] * direction[...]
    for q in range(1, nw):
        copy(part.at[q], part_in.at[q], qs.at[q], qr.at[q], along(q)).wait_recv()
        total = total + part_in[q].astype(jnp.float32)

    def column_sum(x):
        return jnp.sum(x, axis=0, keepdims=True)

    res, direc = residual[...], direction[...]
    at = lax.broadcasted_iota(jnp.int32, (8, res.shape[1]), 0)
    sums = jnp.zeros(at.shape, jnp.float32)
    for k, value in enumerate((res * res, direc * total, res * total, total * total)):
        sums = jnp.where(at == k, column_sum(value), sums)
    stat[...] = sums
    for q in range(1, nw):
        go(copy(stat, stat_z.at[nw - q], zs.at[q], zr.at[nw - q], along(q)))
    for q in range(1, nw):
        copy(stat, stat_z.at[q], zs.at[q], zr.at[q], along(q)).wait_recv()
        sums = sums + stat_z[q]
    stat_o[...] = sums
    for slot in range(1, nb):
        go(copy(stat_o, stat_b.at[back(slot)], bs.at[slot], br.at[back(slot)], plane(slot)))
    for slot in range(1, nb):
        copy(stat_o, stat_b.at[slot], bs.at[slot], br.at[slot], plane(slot)).wait_recv()
        sums = sums + stat_b[slot]
    old_norm, step = sums[0:1], sums[0:1] / sums[1:2]
    new_norm = old_norm - 2.0 * step * sums[2:3] + step * step * sums[3:4]
    new_residual = res - step * total
    residual_out[...] = new_residual
    solution_out[...] = old_solution[...] + step * direc
    direction_out[...] = new_residual + new_norm / old_norm * direc
    for c in sends:
        c.wait_send()


def write_out(a, b, c, a_out, b_out, c_out, sems):
    copies = [
        pltpu.make_async_copy(src, dst, sems.at[k])
        for k, (src, dst) in enumerate(((a, a_out), (b, b_out), (c, c_out)))
    ]
    for copy in copies:
        copy.start()
    for copy in copies:
        copy.wait()


def on_device(nb, nw, points, inv_length, noise_var, solution, residual, direction):
    piece, features = points.shape
    rhs = direction.shape[1]
    vmem = pl.BlockSpec(memory_space=pltpu.VMEM)
    hbm = pl.BlockSpec(memory_space=pl.ANY)
    dma = pltpu.SemaphoreType.DMA
    depth = 3 * features + 2 * TAIL
    common = [
        pltpu.VMEM((features, piece), points.dtype),
        pltpu.VMEM((1, features), jnp.float32),
    ]
    wide = [
        dma((6,)),
        pltpu.VMEM((nb, features + TAIL, piece), jnp.bfloat16),
        pltpu.VMEM((nw, features + TAIL, piece), jnp.bfloat16),
        pltpu.VMEM((nw * piece, depth), jnp.bfloat16),
        pltpu.VMEM((nw * piece, nb * piece), jnp.bfloat16),
        pltpu.VMEM((nb * piece, rhs), jnp.bfloat16),
    ]
    vectors = [pltpu.VMEM((piece, rhs), jnp.float32)] * 3
    parts = [pltpu.VMEM((nw, piece, rhs), jnp.bfloat16)] * 2
    sems = [dma((nb,)), dma((nb,)), dma((nw,)), dma((nw,)), dma((nb,)), dma((nb,)), dma((nw,)), dma((nw,))]
    if nw <= 4:
        body = kernel
        half = rhs // 2
        low = jnp.bfloat16
        scratch = common + [
            pltpu.VMEM((piece, rhs), jnp.float32), pltpu.VMEM((2, piece, rhs), jnp.float32), dma((4,)),
            pltpu.VMEM((nb, features, piece), low), pltpu.VMEM((nw, features, piece), low),
            pltpu.VMEM((nw * piece, depth), low), pltpu.VMEM((nb, depth, piece), low),
            pltpu.VMEM((nw * piece, nb * piece), low),
            pltpu.VMEM((nb, half, piece), low), pltpu.VMEM((nw, half, piece), low),
            pltpu.VMEM((nb * piece, half), low),
            pltpu.VMEM((nw, half, piece), low), pltpu.VMEM((nw, half, piece), low),
            pltpu.VMEM((nb, half, piece), low), pltpu.VMEM((nb, half, piece), low),
            pltpu.VMEM((4, rhs), jnp.float32), pltpu.VMEM((nw * nb, 4, rhs), jnp.float32),
            dma((7,)), dma((nb - 1,)), dma((nw - 1,)), dma((nb // 2,)), dma((4,)),
        ]
    else:
        body = long_kernel
        scratch = common + [pltpu.VMEM((1, 1), jnp.float32)] + vectors + wide + parts + [
            pltpu.VMEM((8, rhs), jnp.float32),
            pltpu.VMEM((nw, 8, rhs), jnp.float32),
            pltpu.VMEM((nb, 8, rhs), jnp.float32),
            pltpu.VMEM((8, rhs), jnp.float32),
        ] + sems + [dma((nw,)), dma((nw,)), dma((nb,)), dma((nb,))]
    news = pl.pallas_call(
        functools.partial(body, nb, nw),
        out_shape=(pltpu.VMEM((piece, rhs), jnp.float32),) * 3,
        in_specs=[hbm, hbm, pl.BlockSpec(memory_space=pltpu.SMEM), hbm, hbm, hbm],
        out_specs=(vmem,) * 3,
        scratch_shapes=scratch,
        compiler_params=pltpu.CompilerParams(
            collective_id=0, has_side_effects=True, vmem_limit_bytes=60 * 1024 * 1024
        ),
    )(points.T, inv_length.reshape(1, features), noise_var.reshape(1, 1), residual, direction, solution)
    return pl.pallas_call(
        write_out,
        out_shape=(jax.ShapeDtypeStruct((piece, rhs), jnp.float32),) * 3,
        in_specs=[vmem] * 3,
        out_specs=(hbm,) * 3,
        scratch_shapes=[dma((3,))],
    )(*(pltpu.with_memory_space_constraint(x, pltpu.VMEM) for x in news))


def solution(mesh):
    spec = P(("blk", "wide"), None)
    return jax.shard_map(
        functools.partial(on_device, mesh.shape["blk"], mesh.shape["wide"]),
        mesh=mesh,
        in_specs=(spec, P(), P(), spec, spec, spec),
        out_specs=(spec, spec, spec),
        check_vma=False,
    )
```

```python
import functools
import math

import jax
import jax.numpy as jnp
from jax import lax
from jax.experimental import pallas as pl
from jax.experimental.pallas import tpu as pltpu
from jax.sharding import PartitionSpec as P

ROOT3 = math.sqrt(3.0)
SCALE = 5.0 / 3.0
MESH = pl.DeviceIdType.MESH
TAIL = 16


def rounded(x):
    return x.astype(jnp.bfloat16).astype(jnp.float32)


def three_parts(x):
    high = rounded(x)
    rest = x - high
    middle = rounded(rest)
    return high, middle, rounded(rest - middle)


def matern(scaled_dist):
    dist = jnp.maximum(scaled_dist, 1e-30)
    root = dist * lax.rsqrt(dist)
    poly = root * (root + ROOT3) + 1.0
    return (poly * jnp.exp2(root * (-ROOT3 / math.log(2.0)))).astype(jnp.bfloat16)


def kernel(nb, nw, points_in, inv_in, noise_in, residual_in, direction_in, solution_in, solution_out, residual_out, direction_out,
           points, inv_length, direction, others, io, feat, feat_z, rows_x, cols_x, kmat, dir_a, dir_b, dir_rows, part_a, part_a_in, part_b, part_b_in, stat, stat_in,
           sent, feat_sem, feat_z_sem, dir_sem, got):
    b = lax.axis_index("blk")
    w = lax.axis_index("wide")
    chips = nb // 2
    chip, core = b // 2, b % 2
    features, piece = points.shape

    def other_chip(k):
        at, bit = chip, 1
        while bit < chips:
            if k & bit:
                at = at + bit - 2 * bit * lax.rem(lax.div(chip, bit), 2)
            bit *= 2
        return at

    def same_core(k):
        return (other_chip(k) * 2 + core, w)

    sibling = (chip * 2 + 1 - core, w)

    def along(q):
        return (b, lax.rem(w + q, nw))

    def at_least(limit):
        return lax.div(w + nw - limit, nw)

    upper = lax.div(2 * w, nw)

    def far_first(k):
        low = nw - 1 - k - at_least(nw - 1 - k)
        high = k + 1 - at_least(k + 1)
        return lax.rem(low + upper * (high - low) - w + nw, nw)

    z_far = [far_first(k) for k in range(nw - 1)]
    chips_far = sorted(range(1, chips), key=lambda k: -bin(k).count("1"))
    chips_near = chips_far[::-1]

    def copy(src, dst, send, recv, to):
        return pltpu.make_async_remote_copy(
            src_ref=src, dst_ref=dst, send_sem=send, recv_sem=recv, device_id=to, device_id_type=MESH
        )

    loads = [
        pltpu.make_async_copy(src, dst, io.at[min(k, 3)])
        for k, (src, dst) in enumerate(
            ((points_in, points), (inv_in, inv_length), (direction_in, direction),
             (residual_in, others.at[0]), (solution_in, others.at[1]))
        )
    ]
    for load in loads[:2]:
        load.start()
    barrier = pltpu.get_barrier_semaphore()
    for q in z_far:
        pl.semaphore_signal(barrier, inc=1, device_id=along(q), device_id_type=MESH)
    for k in chips_far:
        pl.semaphore_signal(barrier, inc=1, device_id=same_core(k), device_id_type=MESH)
    pl.semaphore_signal(barrier, inc=1, device_id=sibling, device_id_type=MESH)
    for load in loads[2:]:
        load.start()
    for load in loads[:2]:
        load.wait()

    inv_row = jnp.concatenate(
        [inv_length[...], jnp.zeros((1, 128 - features), jnp.float32)], axis=1)
    inv_column = jnp.broadcast_to(inv_row, (8, 128)).T[:features, 0:1]
    x_t = rounded(points[...].astype(jnp.float32) * inv_column)
    feat[0] = x_t.astype(jnp.bfloat16)
    pl.semaphore_wait(barrier, chips + nw - 1)

    DIR_Z, PART, PART_Z, STAT, FEAT, FEAT_Z, DIR = range(7)

    def feat_copy(src_slot, dst_slot, to):
        return copy(feat.at[src_slot], feat.at[dst_slot], sent.at[FEAT], feat_sem.at[dst_slot - 1], to)

    def dir_copy(src_slot, dst_slot, to):
        return copy(dir_a.at[src_slot], dir_a.at[dst_slot], sent.at[DIR], dir_sem.at[min(dst_slot, chips) - 1], to)

    def feat_z_copy(src, slot, q):
        return copy(src, feat_z.at[slot], sent.at[FEAT_Z], feat_z_sem.at[slot - 1], along(q))

    for q in z_far:
        feat_z_copy(feat.at[0], nw - q, q).start()
    feat_copy(0, chips, sibling).start()
    for k in chips_near:
        feat_copy(0, k, same_core(k)).start()
    loads[2].wait()
    dir_t = direction[...].T.astype(jnp.bfloat16)
    part = dir_t.shape[0] // 2
    dir_a[0] = dir_t[:part]
    dir_b[0] = dir_t[part:]
    for k in chips_far:
        dir_copy(0, k, same_core(k)).start()
    dir_copy(0, chips, sibling).start()
    dir_rows[0:piece] = direction[...][:, :part].astype(jnp.bfloat16)

    def feat_arrived(slot):
        feat_copy(slot, slot, sibling).wait_recv()

    def relay_feat(k):
        feat_arrived(k)
        feat_copy(k, chips + k, sibling).start()

    def turn(slot):
        dir_rows[at_rows(slot), :] = dir_a[slot].astype(jnp.float32).T.astype(jnp.bfloat16)

    def relay_dir(k):
        dir_copy(k, k, sibling).wait_recv()
        dir_copy(k, chips + k, sibling).start()

    depth = rows_x.shape[1]
    ones = jnp.where(lax.broadcasted_iota(jnp.int32, (8, piece), 0) < 3, 1.0, 0.0)
    at = lax.broadcasted_iota(jnp.int32, (8, piece), 0)
    blank = jnp.zeros((depth - 3 * features - 16, piece), jnp.float32)

    def norms(x, first):
        result = jnp.zeros((8, piece), jnp.float32)
        for k, value in enumerate(three_parts(SCALE * jnp.sum(x * x, axis=0, keepdims=True))):
            result = jnp.where(at == first + k, value, result)
        return result

    def make_rows(j, block):
        x = block.astype(jnp.float32)
        lanes = jnp.concatenate(
            [-2.0 * value for value in three_parts(SCALE * x)] + [ones, norms(x, 0), blank], axis=0)
        rows_x[j * piece : (j + 1) * piece] = lanes.T.astype(jnp.bfloat16)

    def make_cols(slot):
        block = feat[slot]
        tail = jnp.concatenate([norms(block.astype(jnp.float32), 0), ones, blank], axis=0)
        cols_x[slot] = jnp.concatenate([block] * 3 + [tail.astype(jnp.bfloat16)], axis=0)

    start = lax.div(w, nw)

    def stored(j, count=1):
        return pl.ds(pl.multiple_of((start + j) * piece, piece), count * piece)

    def at_rows(j):
        return slice(j * piece, (j + 1) * piece)

    z_near = [0] + z_far[::-1]

    have_rows, have_cols, due = [], [], []

    def flush():
        for j, slot in due:
            dist = jnp.dot(rows_x[at_rows(j), :], cols_x[slot], preferred_element_type=jnp.float32)
            kmat[at_rows(j), at_rows(slot)] = matern(dist)
        due.clear()

    def add_rows(j):
        if j:
            q = z_near[j]
            feat_z_copy(feat_z.at[q], q, q).wait_recv()
            make_rows(j, feat_z[q])
        else:
            make_rows(0, feat[0])
        flush()
        due.extend((j, slot) for slot in have_cols)
        have_rows.append(j)

    def add_cols(slot):
        if slot >= chips:
            feat_arrived(slot)
        make_cols(slot)
        flush()
        due.extend((j, slot) for j in have_rows)
        have_cols.append(slot)

    every = range(nw)
    near, last = chips_near[:-1], chips_near[-1:]
    add_rows(0)
    add_cols(0)
    add_cols(chips)
    flush()
    for q in z_far:
        copy(dir_b.at[0], dir_b.at[nw - q], sent.at[DIR_Z], got.at[DIR_Z], along(q)).start()
    for k in near:
        relay_feat(k)
    for k in near:
        add_cols(k)
    if nw > 1:
        add_rows(1)
    for k in last:
        relay_feat(k)
        add_cols(k)
    for k in near:
        add_cols(chips + k)
    for k in near:
        relay_dir(k)
    for j in range(2, nw - 1):
        add_rows(j)
    for k in last:
        relay_dir(k)
    for j in range(max(2, nw - 1), nw):
        add_rows(j)
    for k in last:
        add_cols(chips + k)
    for k in range(1, chips):
        turn(k)
    flush()

    def product_a(rows):
        product = jnp.dot(kmat[stored(rows[0], len(rows)), :], dir_rows[...], preferred_element_type=jnp.float32)
        return {j: product[at * piece : (at + 1) * piece].T for at, j in enumerate(rows)}

    def product_b(slot):
        total = None
        for j in every:
            term = jnp.dot(dir_b[z_near[j]], kmat[stored(j), at_rows(slot)],
                           preferred_element_type=jnp.float32)
            total = term if total is None else total + term
        return total

    def send_a(j, value):
        q = z_near[j]
        part_a[j] = value.astype(jnp.bfloat16)
        copy(part_a.at[j], part_a_in.at[nw - q], sent.at[PART_Z], got.at[PART_Z], along(q)).start()

    def send_b(k, c, value):
        slot = c * chips + k
        to = (other_chip(k) * 2 + (1 - core if c else core), w)
        part_b[slot] = value.astype(jnp.bfloat16)
        copy(part_b.at[slot], part_b_in.at[slot], sent.at[PART], got.at[PART], to).start()

    def all_of(ref, kind, recv):
        return copy(ref, ref, sent.at[kind], recv, sibling)

    relayed, z_dirs = dir_a.at[pl.ds(chips, chips)], dir_b.at[pl.ds(1, nw - 1)]
    all_of(relayed, DIR, dir_sem.at[chips - 1]).wait_recv()
    for k in range(chips):
        turn(chips + k)
    all_of(z_dirs, DIR_Z, got.at[DIR_Z]).wait_recv()
    for step, k in enumerate(chips_far + [0] + [None] * (nw - chips)):
        j = nw - 1 - step
        if j > 0:
            found = product_a([j])[j]
        if k is not None:
            pair = [product_b(k), product_b(chips + k)]
        if j > 0:
            send_a(j, found)
        if k:
            send_b(k, 0, pair[0])
        elif k == 0:
            total_b = pair[0]
        if k is not None:
            send_b(k, 1, pair[1])
    total_a = product_a([0])[0]
    parts_z, parts_b = part_a_in.at[pl.ds(1, nw - 1)], part_b_in.at[pl.ds(1, nb - 1)]
    all_of(parts_z, PART_Z, got.at[PART_Z]).wait_recv()
    for q in range(1, nw):
        total_a = total_a + part_a_in[q].astype(jnp.float32)
    all_of(parts_b, PART, got.at[PART]).wait_recv()
    for slot in range(1, nb):
        total_b = total_b + part_b_in[slot].astype(jnp.float32)
    make_vectors = pltpu.make_async_copy(others, others, io.at[3])
    make_vectors.wait()
    res, direc = others[0], direction[...]
    total = jnp.concatenate([total_a, total_b], axis=0).T + noise_in[0, 0] * direc

    for k, value in enumerate((res * res, direc * total, res * total, total * total)):
        stat[k : k + 1] = jnp.sum(value, axis=0, keepdims=True)
    for r, q in enumerate(z_far + [0]):
        for k in chips_far + [0]:
            for c in range(2):
                if r == nw - 1 and k == 0 and c == 0:
                    continue
                to = (other_chip(k) * 2 + (core if c == 0 else 1 - core), lax.rem(w + q, nw))
                slot = (lax.rem(nw - q, nw) * 2 + c) * chips + k
                copy(stat, stat_in.at[slot], sent.at[STAT], got.at[STAT], to).start()
    stats = stat_in.at[pl.ds(1, nb * nw - 1)]
    all_of(stats, STAT, got.at[STAT]).wait_recv()
    sums = stat[...]
    for slot in range(1, nb * nw):
        sums = sums + stat_in[slot]
    old_norm, step = sums[0:1], sums[0:1] / sums[1:2]
    new_norm = old_norm - 2.0 * step * sums[2:3] + step * step * sums[3:4]
    new_residual = res - step * total
    residual_out[...] = new_residual
    solution_out[...] = others[1] + step * direc
    direction_out[...] = new_residual + new_norm / old_norm * direc
    for ref, kind in ((feat.at[pl.ds(1, nb - 1)], FEAT), (feat_z.at[pl.ds(1, nw - 1)], FEAT_Z), (dir_a.at[pl.ds(1, nb - 1)], DIR),
                      (z_dirs, DIR_Z), (parts_b, PART), (parts_z, PART_Z), (stats, STAT)):
        all_of(ref, kind, got.at[STAT]).wait_send()


def long_kernel(nb, nw, points_in, inv_in, noise_in, residual_in, direction_in, solution_in, solution_out, residual_out, direction_out,
           points, inv_length, noise_var, residual, direction, old_solution, io, feat, feat_z, rows_x, kmat, low_dir, part, part_in, stat, stat_z, stat_b, stat_o,
           fs, fr, fzs, fzr, ps, pr, qs, qr, zs, zr, bs, br):
    b = lax.axis_index("blk")
    w = lax.axis_index("wide")
    chips = nb // 2
    chip, core = b // 2, b % 2
    features, piece = points.shape

    def same_core(q):
        return (lax.rem(chip + q, chips) * 2 + core, w)

    sibling = (chip * 2 + 1 - core, w)

    def along(q):
        return (b, lax.rem(w + q, nw))

    def plane(slot):
        return (lax.rem(chip + slot // 2, chips) * 2 + (core if slot % 2 == 0 else 1 - core), w)

    def back(slot):
        return (chips - slot // 2) % chips * 2 + slot % 2

    barrier = pltpu.get_barrier_semaphore()
    for slot in range(1, nb):
        pl.semaphore_signal(barrier, inc=1, device_id=plane(slot), device_id_type=MESH)
    for q in range(1, nw):
        pl.semaphore_signal(barrier, inc=1, device_id=along(q), device_id_type=MESH)

    def copy(src, dst, send, recv, to):
        return pltpu.make_async_remote_copy(
            src_ref=src, dst_ref=dst, send_sem=send, recv_sem=recv, device_id=to, device_id_type=MESH
        )

    loads = [
        pltpu.make_async_copy(src, dst, io.at[k])
        for k, (src, dst) in enumerate(
            ((points_in, points), (inv_in, inv_length), (direction_in, direction),
             (residual_in, residual), (solution_in, old_solution))
        )
    ]
    for load in loads:
        load.start()
    for load in loads[:2]:
        load.wait()

    inv_row = jnp.concatenate(
        [inv_length[...], jnp.zeros((1, 128 - features), jnp.float32)], axis=1)
    inv_column = jnp.broadcast_to(inv_row, (8, 128)).T[:features, 0:1]
    x_t = rounded(points[...].astype(jnp.float32) * inv_column)
    s1, s2, s3 = three_parts(SCALE * jnp.sum(x_t * x_t, axis=0, keepdims=True))
    row = lax.broadcasted_iota(jnp.int32, (TAIL, piece), 0)
    tail = jnp.where((row >= 3) & (row <= 10), 1.0, 0.0)
    tail = jnp.where((row >= 6) & (row <= 7), 0.0, tail)
    for at, value in ((0, s1), (1, s2), (2, s3), (11, s1), (12, s2), (13, s3)):
        tail = jnp.where(row == at, value, tail)
    feat[0] = jnp.concatenate([x_t, tail], axis=0).astype(jnp.bfloat16)
    for load in loads[2:]:
        load.wait()
    low_dir[0:piece] = direction[...].astype(jnp.bfloat16)
    pl.semaphore_wait(barrier, nb - 1 + nw - 1)

    upper = lax.div(2 * w, nw)

    def near(k):
        return k + upper * (nw - 2 * k)

    def rows_at(q):
        return pl.ds(pl.multiple_of(q * piece, piece), piece)

    sends = []

    def go(c):
        c.start()
        sends.append(c)
        return c

    def feat_copy(src_slot, dst_slot, to):
        return copy(feat.at[src_slot], feat.at[dst_slot], fs.at[dst_slot], fr.at[dst_slot], to)

    def dir_copy(src_slot, dst_slot, to):
        return copy(low_dir.at[pl.ds(src_slot * piece, piece)], low_dir.at[pl.ds(dst_slot * piece, piece)],
                    ps.at[dst_slot], pr.at[dst_slot], to)

    for k in range(1, nw):
        q = near(nw - k)
        go(copy(feat.at[0], feat_z.at[nw - q], fzs.at[q], fzr.at[nw - q], along(q)))
    go(feat_copy(0, 1, sibling))
    for q in range(1, chips):
        go(feat_copy(0, 2 * (chips - q), same_core(q)))
    for q in range(1, chips):
        go(dir_copy(0, 2 * (chips - q), same_core(q)))
    go(dir_copy(0, 1, sibling))

    def feat_arrived(slot):
        feat_copy(slot, slot, sibling).wait_recv()

    def dir_arrived(slot):
        dir_copy(slot, slot, sibling).wait_recv()

    def as_rows(block):
        block = block.astype(jnp.float32)
        x = block[:features]
        h, m, l = three_parts(SCALE * x)
        lanes = jnp.concatenate(
            [-2.0 * h, -2.0 * m, -2.0 * l, block[features + 8 :],
             jnp.zeros((TAIL + 8, piece), jnp.float32)], axis=0)
        return lanes.T.astype(jnp.bfloat16)

    depth = rows_x.shape[1]

    def tile(at, slot):
        block = feat[slot]
        cols = jnp.concatenate(
            [block[:features]] * 3 + [block[features:],
             jnp.zeros((depth - 3 * features - TAIL, piece), jnp.bfloat16)], axis=0)
        dist = jnp.dot(rows_x[at, :], cols, preferred_element_type=jnp.float32)
        kmat[at, slot * piece : (slot + 1) * piece] = matern(dist)

    def feat_z_arrived(q):
        copy(feat_z.at[q], feat_z.at[q], fzs.at[q], fzr.at[q], along(q)).wait_recv()

    def relay_direction(q):
        dir_arrived(2 * q)
        go(dir_copy(2 * q, 2 * q + 1, sibling))

    rows_x[0:piece] = as_rows(feat[0])
    tile(pl.ds(0, piece), 0)
    feat_arrived(1)
    tile(pl.ds(0, piece), 1)
    for q in range(1, chips):
        feat_arrived(2 * q)
        go(feat_copy(2 * q, 2 * q + 1, sibling))
        tile(pl.ds(0, piece), 2 * q)
    for q in range(1, chips):
        feat_arrived(2 * q + 1)
        tile(pl.ds(0, piece), 2 * q + 1)
    if nw <= 4:
        relayed = 1
        for k in range(1, nw):
            q = near(k)
            feat_z_arrived(q)
            rows_x[rows_at(q), :] = as_rows(feat_z[q])
            for slot in range(nb):
                tile(rows_at(q), slot)
                if k == nw - 1 and slot in (0, nb // 2) and relayed < chips:
                    relay_direction(relayed)
                    relayed += 1
    else:
        relayed = 1
        for q in range(1, nw):
            feat_z_arrived(q)
            rows_x[q * piece : (q + 1) * piece] = as_rows(feat_z[q])

        def row_tiles(q, carry):
            for slot in range(nb):
                tile(pl.ds(pl.multiple_of(q * piece, piece), piece), slot)
            return carry

        lax.fori_loop(1, nw, row_tiles, 0)
    for q in range(relayed, chips):
        relay_direction(q)
    for q in range(chips):
        dir_arrived(2 * q + 1)

    def partial(q):
        return jnp.dot(kmat[rows_at(q), :], low_dir[...],
                       preferred_element_type=jnp.float32)

    for k in range(1, nw):
        q = near(nw - k)
        part[q] = partial(q).astype(jnp.bfloat16)
        go(copy(part.at[q], part_in.at[nw - q], qs.at[q], qr.at[nw - q], along(q)))
    total = partial(0) + noise_in[0, 0] * direction[...]
    for q in range(1, nw):
        copy(part.at[q], part_in.at[q], qs.at[q], qr.at[q], along(q)).wait_recv()
        total = total + part_in[q].astype(jnp.float32)

    def column_sum(x):
        return jnp.sum(x, axis=0, keepdims=True)

    res, direc = residual[...], direction[...]
    at = lax.broadcasted_iota(jnp.int32, (8, res.shape[1]), 0)
    sums = jnp.zeros(at.shape, jnp.float32)
    for k, value in enumerate((res * res, direc * total, res * total, total * total)):
        sums = jnp.where(at == k, column_sum(value), sums)
    stat[...] = sums
    for q in range(1, nw):
        go(copy(stat, stat_z.at[nw - q], zs.at[q], zr.at[nw - q], along(q)))
    for q in range(1, nw):
        copy(stat, stat_z.at[q], zs.at[q], zr.at[q], along(q)).wait_recv()
        sums = sums + stat_z[q]
    stat_o[...] = sums
    for slot in range(1, nb):
        go(copy(stat_o, stat_b.at[back(slot)], bs.at[slot], br.at[back(slot)], plane(slot)))
    for slot in range(1, nb):
        copy(stat_o, stat_b.at[slot], bs.at[slot], br.at[slot], plane(slot)).wait_recv()
        sums = sums + stat_b[slot]
    old_norm, step = sums[0:1], sums[0:1] / sums[1:2]
    new_norm = old_norm - 2.0 * step * sums[2:3] + step * step * sums[3:4]
    new_residual = res - step * total
    residual_out[...] = new_residual
    solution_out[...] = old_solution[...] + step * direc
    direction_out[...] = new_residual + new_norm / old_norm * direc
    for c in sends:
        c.wait_send()


def write_out(a, b, c, a_out, b_out, c_out, sems):
    copies = [
        pltpu.make_async_copy(src, dst, sems.at[k])
        for k, (src, dst) in enumerate(((a, a_out), (b, b_out), (c, c_out)))
    ]
    for copy in copies:
        copy.start()
    for copy in copies:
        copy.wait()


def on_device(nb, nw, points, inv_length, noise_var, solution, residual, direction):
    piece, features = points.shape
    rhs = direction.shape[1]
    vmem = pl.BlockSpec(memory_space=pltpu.VMEM)
    hbm = pl.BlockSpec(memory_space=pl.ANY)
    dma = pltpu.SemaphoreType.DMA
    depth = 3 * features + 2 * TAIL
    common = [
        pltpu.VMEM((features, piece), points.dtype),
        pltpu.VMEM((1, features), jnp.float32),
    ]
    wide = [
        dma((6,)),
        pltpu.VMEM((nb, features + TAIL, piece), jnp.bfloat16),
        pltpu.VMEM((nw, features + TAIL, piece), jnp.bfloat16),
        pltpu.VMEM((nw * piece, depth), jnp.bfloat16),
        pltpu.VMEM((nw * piece, nb * piece), jnp.bfloat16),
        pltpu.VMEM((nb * piece, rhs), jnp.bfloat16),
    ]
    vectors = [pltpu.VMEM((piece, rhs), jnp.float32)] * 3
    parts = [pltpu.VMEM((nw, piece, rhs), jnp.bfloat16)] * 2
    sems = [dma((nb,)), dma((nb,)), dma((nw,)), dma((nw,)), dma((nb,)), dma((nb,)), dma((nw,)), dma((nw,))]
    if nw <= 4:
        body = kernel
        half = rhs // 2
        low = jnp.bfloat16
        scratch = common + [
            pltpu.VMEM((piece, rhs), jnp.float32), pltpu.VMEM((2, piece, rhs), jnp.float32), dma((4,)),
            pltpu.VMEM((nb, features, piece), low), pltpu.VMEM((nw, features, piece), low),
            pltpu.VMEM((nw * piece, depth), low), pltpu.VMEM((nb, depth, piece), low),
            pltpu.VMEM((nw * piece, nb * piece), low),
            pltpu.VMEM((nb, half, piece), low), pltpu.VMEM((nw, half, piece), low),
            pltpu.VMEM((nb * piece, half), low),
            pltpu.VMEM((nw, half, piece), low), pltpu.VMEM((nw, half, piece), low),
            pltpu.VMEM((nb, half, piece), low), pltpu.VMEM((nb, half, piece), low),
            pltpu.VMEM((4, rhs), jnp.float32), pltpu.VMEM((nw * nb, 4, rhs), jnp.float32),
            dma((7,)), dma((nb - 1,)), dma((nw - 1,)), dma((nb // 2,)), dma((4,)),
        ]
    else:
        body = long_kernel
        scratch = common + [pltpu.VMEM((1, 1), jnp.float32)] + vectors + wide + parts + [
            pltpu.VMEM((8, rhs), jnp.float32),
            pltpu.VMEM((nw, 8, rhs), jnp.float32),
            pltpu.VMEM((nb, 8, rhs), jnp.float32),
            pltpu.VMEM((8, rhs), jnp.float32),
        ] + sems + [dma((nw,)), dma((nw,)), dma((nb,)), dma((nb,))]
    news = pl.pallas_call(
        functools.partial(body, nb, nw),
        out_shape=(pltpu.VMEM((piece, rhs), jnp.float32),) * 3,
        in_specs=[hbm, hbm, pl.BlockSpec(memory_space=pltpu.SMEM), hbm, hbm, hbm],
        out_specs=(vmem,) * 3,
        scratch_shapes=scratch,
        compiler_params=pltpu.CompilerParams(
            collective_id=0, has_side_effects=True, vmem_limit_bytes=60 * 1024 * 1024
        ),
    )(points.T, inv_length.reshape(1, features), noise_var.reshape(1, 1), residual, direction, solution)
    return pl.pallas_call(
        write_out,
        out_shape=(jax.ShapeDtypeStruct((piece, rhs), jnp.float32),) * 3,
        in_specs=[vmem] * 3,
        out_specs=(hbm,) * 3,
        scratch_shapes=[dma((3,))],
    )(*(pltpu.with_memory_space_constraint(x, pltpu.VMEM) for x in news))


def solution(mesh):
    spec = P(("blk", "wide"), None)
    return jax.shard_map(
        functools.partial(on_device, mesh.shape["blk"], mesh.shape["wide"]),
        mesh=mesh,
        in_specs=(spec, P(), P(), spec, spec, spec),
        out_specs=(spec, spec, spec),
        check_vma=False,
    )
```

```python
import functools
import math

import jax
import jax.numpy as jnp
from jax import lax
from jax.experimental import pallas as pl
from jax.experimental.pallas import tpu as pltpu
from jax.sharding import PartitionSpec as P

ROOT3 = math.sqrt(3.0)
SCALE = 5.0 / 3.0
MESH = pl.DeviceIdType.MESH
TAIL = 16


def rounded(x):
    return x.astype(jnp.bfloat16).astype(jnp.float32)


def three_parts(x):
    high = rounded(x)
    rest = x - high
    middle = rounded(rest)
    return high, middle, rounded(rest - middle)


def matern(scaled_dist):
    dist = jnp.maximum(scaled_dist, 1e-30)
    root = dist * lax.rsqrt(dist)
    poly = root * (root + ROOT3) + 1.0
    return (poly * jnp.exp2(root * (-ROOT3 / math.log(2.0)))).astype(jnp.bfloat16)


def kernel(nb, nw, points_in, inv_in, noise_in, residual_in, direction_in, solution_in, solution_out, residual_out, direction_out,
           points, inv_length, direction, others, io, feat, feat_z, rows_x, cols_x, kmat, dir_a, dir_b, dir_rows, part_a, part_a_in, part_b, part_b_in, stat, stat_in,
           sent, feat_sem, feat_z_sem, dir_sem, got):
    b = lax.axis_index("blk")
    w = lax.axis_index("wide")
    chips = nb // 2
    chip, core = b // 2, b % 2
    features, piece = points.shape

    def other_chip(k):
        at, bit = chip, 1
        while bit < chips:
            if k & bit:
                at = at + bit - 2 * bit * lax.rem(lax.div(chip, bit), 2)
            bit *= 2
        return at

    def same_core(k):
        return (other_chip(k) * 2 + core, w)

    sibling = (chip * 2 + 1 - core, w)

    def along(q):
        return (b, lax.rem(w + q, nw))

    def at_least(limit):
        return lax.div(w + nw - limit, nw)

    upper = lax.div(2 * w, nw)

    def far_first(k):
        low = nw - 1 - k - at_least(nw - 1 - k)
        high = k + 1 - at_least(k + 1)
        return lax.rem(low + upper * (high - low) - w + nw, nw)

    z_far = [far_first(k) for k in range(nw - 1)]
    chips_far = sorted(range(1, chips), key=lambda k: -bin(k).count("1"))
    chips_near = chips_far[::-1]

    def copy(src, dst, send, recv, to):
        return pltpu.make_async_remote_copy(
            src_ref=src, dst_ref=dst, send_sem=send, recv_sem=recv, device_id=to, device_id_type=MESH
        )

    loads = [
        pltpu.make_async_copy(src, dst, io.at[min(k, 3)])
        for k, (src, dst) in enumerate(
            ((points_in, points), (inv_in, inv_length), (direction_in, direction),
             (residual_in, others.at[0]), (solution_in, others.at[1]))
        )
    ]
    for load in loads[:2]:
        load.start()
    barrier = pltpu.get_barrier_semaphore()
    for q in z_far:
        pl.semaphore_signal(barrier, inc=1, device_id=along(q), device_id_type=MESH)
    for k in chips_far:
        pl.semaphore_signal(barrier, inc=1, device_id=same_core(k), device_id_type=MESH)
    pl.semaphore_signal(barrier, inc=1, device_id=sibling, device_id_type=MESH)
    for load in loads[2:]:
        load.start()
    for load in loads[:2]:
        load.wait()

    inv_row = jnp.concatenate(
        [inv_length[...], jnp.zeros((1, 128 - features), jnp.float32)], axis=1)
    inv_column = jnp.broadcast_to(inv_row, (8, 128)).T[:features, 0:1]
    x_t = rounded(points[...].astype(jnp.float32) * inv_column)
    feat[0] = x_t.astype(jnp.bfloat16)
    pl.semaphore_wait(barrier, chips + nw - 1)

    DIR_Z, PART, PART_Z, STAT, FEAT, FEAT_Z, DIR = range(7)

    def feat_copy(src_slot, dst_slot, to):
        return copy(feat.at[src_slot], feat.at[dst_slot], sent.at[FEAT], feat_sem.at[dst_slot - 1], to)

    def dir_copy(src_slot, dst_slot, to):
        return copy(dir_a.at[src_slot], dir_a.at[dst_slot], sent.at[DIR], dir_sem.at[min(dst_slot, chips) - 1], to)

    def feat_z_copy(src, slot, q):
        return copy(src, feat_z.at[slot], sent.at[FEAT_Z], feat_z_sem.at[slot - 1], along(q))

    for q in z_far:
        feat_z_copy(feat.at[0], nw - q, q).start()
    feat_copy(0, chips, sibling).start()
    for k in chips_near:
        feat_copy(0, k, same_core(k)).start()
    loads[2].wait()
    dir_t = direction[...].T.astype(jnp.bfloat16)
    part = dir_t.shape[0] // 2
    dir_a[0] = dir_t[:part]
    dir_b[0] = dir_t[part:]
    for k in chips_far:
        dir_copy(0, k, same_core(k)).start()
    dir_copy(0, chips, sibling).start()
    dir_rows[0:piece] = direction[...][:, :part].astype(jnp.bfloat16)

    def feat_arrived(slot):
        feat_copy(slot, slot, sibling).wait_recv()

    def relay_feat(k):
        feat_arrived(k)
        feat_copy(k, chips + k, sibling).start()

    def turn(slot):
        dir_rows[at_rows(slot), :] = dir_a[slot].astype(jnp.float32).T.astype(jnp.bfloat16)

    def relay_dir(k):
        dir_copy(k, k, sibling).wait_recv()
        dir_copy(k, chips + k, sibling).start()

    depth = rows_x.shape[1]
    ones = jnp.where(lax.broadcasted_iota(jnp.int32, (8, piece), 0) < 3, 1.0, 0.0)
    at = lax.broadcasted_iota(jnp.int32, (8, piece), 0)
    blank = jnp.zeros((depth - 3 * features - 16, piece), jnp.float32)

    def norms(x, first):
        result = jnp.zeros((8, piece), jnp.float32)
        for k, value in enumerate(three_parts(SCALE * jnp.sum(x * x, axis=0, keepdims=True))):
            result = jnp.where(at == first + k, value, result)
        return result

    def make_rows(j, block):
        x = block.astype(jnp.float32)
        lanes = jnp.concatenate(
            [-2.0 * value for value in three_parts(SCALE * x)] + [ones, norms(x, 0), blank], axis=0)
        rows_x[j * piece : (j + 1) * piece] = lanes.T.astype(jnp.bfloat16)

    def make_cols(slot):
        block = feat[slot]
        tail = jnp.concatenate([norms(block.astype(jnp.float32), 0), ones, blank], axis=0)
        cols_x[slot] = jnp.concatenate([block] * 3 + [tail.astype(jnp.bfloat16)], axis=0)

    start = lax.div(w, nw)

    def stored(j, count=1):
        return pl.ds(pl.multiple_of((start + j) * piece, piece), count * piece)

    def at_rows(j):
        return slice(j * piece, (j + 1) * piece)

    z_near = [0] + z_far[::-1]

    have_rows, have_cols, due = [], [], []

    def flush():
        for j, slot in due:
            dist = jnp.dot(rows_x[at_rows(j), :], cols_x[slot], preferred_element_type=jnp.float32)
            kmat[at_rows(j), at_rows(slot)] = matern(dist)
        due.clear()

    def add_rows(j):
        if j:
            q = z_near[j]
            feat_z_copy(feat_z.at[q], q, q).wait_recv()
            make_rows(j, feat_z[q])
        else:
            make_rows(0, feat[0])
        flush()
        due.extend((j, slot) for slot in have_cols)
        have_rows.append(j)

    def add_cols(slot):
        if slot >= chips:
            feat_arrived(slot)
        make_cols(slot)
        flush()
        due.extend((j, slot) for j in have_rows)
        have_cols.append(slot)

    every = range(nw)
    near, last = chips_near[:-1], chips_near[-1:]
    add_rows(0)
    add_cols(0)
    add_cols(chips)
    flush()
    for q in z_far:
        copy(dir_b.at[0], dir_b.at[nw - q], sent.at[DIR_Z], got.at[DIR_Z], along(q)).start()
    for k in near:
        relay_feat(k)
    for k in near:
        add_cols(k)
    if nw > 1:
        add_rows(1)
    for k in last:
        relay_feat(k)
        add_cols(k)
    for k in near:
        add_cols(chips + k)
    for k in near:
        relay_dir(k)
    for j in range(2, nw - 1):
        add_rows(j)
    for k in last:
        relay_dir(k)
    for j in range(max(2, nw - 1), nw):
        add_rows(j)
    for k in last:
        add_cols(chips + k)
    for k in range(1, chips):
        turn(k)
    flush()

    def product_a(rows):
        product = jnp.dot(kmat[stored(rows[0], len(rows)), :], dir_rows[...], preferred_element_type=jnp.float32)
        return {j: product[at * piece : (at + 1) * piece].T for at, j in enumerate(rows)}

    def product_b(slot):
        total = None
        for j in every:
            term = jnp.dot(dir_b[z_near[j]], kmat[stored(j), at_rows(slot)],
                           preferred_element_type=jnp.float32)
            total = term if total is None else total + term
        return total

    def send_a(j, value):
        q = z_near[j]
        part_a[j] = value.astype(jnp.bfloat16)
        copy(part_a.at[j], part_a_in.at[nw - q], sent.at[PART_Z], got.at[PART_Z], along(q)).start()

    def send_b(k, c, value):
        slot = c * chips + k
        to = (other_chip(k) * 2 + (1 - core if c else core), w)
        part_b[slot] = value.astype(jnp.bfloat16)
        copy(part_b.at[slot], part_b_in.at[slot], sent.at[PART], got.at[PART], to).start()

    def all_of(ref, kind, recv):
        return copy(ref, ref, sent.at[kind], recv, sibling)

    relayed, z_dirs = dir_a.at[pl.ds(chips, chips)], dir_b.at[pl.ds(1, nw - 1)]
    all_of(relayed, DIR, dir_sem.at[chips - 1]).wait_recv()
    for k in range(chips):
        turn(chips + k)
    all_of(z_dirs, DIR_Z, got.at[DIR_Z]).wait_recv()
    for step, k in enumerate(chips_far + [0] + [None] * (nw - chips)):
        j = nw - 1 - step
        if j > 0:
            found = product_a([j])[j]
        if k is not None:
            pair = [product_b(k), product_b(chips + k)]
        if k:
            send_b(k, 0, pair[0])
        if j > 0:
            send_a(j, found)
        if k == 0:
            total_b = pair[0]
        if k is not None:
            send_b(k, 1, pair[1])
    total_a = product_a([0])[0]
    parts_z, parts_b = part_a_in.at[pl.ds(1, nw - 1)], part_b_in.at[pl.ds(1, nb - 1)]
    all_of(parts_z, PART_Z, got.at[PART_Z]).wait_recv()
    for q in range(1, nw):
        total_a = total_a + part_a_in[q].astype(jnp.float32)
    all_of(parts_b, PART, got.at[PART]).wait_recv()
    for slot in range(1, nb):
        total_b = total_b + part_b_in[slot].astype(jnp.float32)
    make_vectors = pltpu.make_async_copy(others, others, io.at[3])
    make_vectors.wait()
    res, direc = others[0], direction[...]
    total = jnp.concatenate([total_a, total_b], axis=0).T + noise_in[0, 0] * direc

    for k, value in enumerate((res * res, direc * total, res * total, total * total)):
        stat[k : k + 1] = jnp.sum(value, axis=0, keepdims=True)
    for r, q in enumerate(z_far + [0]):
        for k in chips_far + [0]:
            for c in range(2):
                if r == nw - 1 and k == 0 and c == 0:
                    continue
                to = (other_chip(k) * 2 + (core if c == 0 else 1 - core), lax.rem(w + q, nw))
                slot = (lax.rem(nw - q, nw) * 2 + c) * chips + k
                copy(stat, stat_in.at[slot], sent.at[STAT], got.at[STAT], to).start()
    stats = stat_in.at[pl.ds(1, nb * nw - 1)]
    all_of(stats, STAT, got.at[STAT]).wait_recv()
    sums = stat[...]
    for slot in range(1, nb * nw):
        sums = sums + stat_in[slot]
    old_norm, step = sums[0:1], sums[0:1] / sums[1:2]
    new_norm = old_norm - 2.0 * step * sums[2:3] + step * step * sums[3:4]
    new_residual = res - step * total
    residual_out[...] = new_residual
    solution_out[...] = others[1] + step * direc
    direction_out[...] = new_residual + new_norm / old_norm * direc
    for ref, kind in ((feat.at[pl.ds(1, nb - 1)], FEAT), (feat_z.at[pl.ds(1, nw - 1)], FEAT_Z), (dir_a.at[pl.ds(1, nb - 1)], DIR),
                      (z_dirs, DIR_Z), (parts_b, PART), (parts_z, PART_Z), (stats, STAT)):
        all_of(ref, kind, got.at[STAT]).wait_send()


def long_kernel(nb, nw, points_in, inv_in, noise_in, residual_in, direction_in, solution_in, solution_out, residual_out, direction_out,
           points, inv_length, noise_var, residual, direction, old_solution, io, feat, feat_z, rows_x, kmat, low_dir, part, part_in, stat, stat_z, stat_b, stat_o,
           fs, fr, fzs, fzr, ps, pr, qs, qr, zs, zr, bs, br):
    b = lax.axis_index("blk")
    w = lax.axis_index("wide")
    chips = nb // 2
    chip, core = b // 2, b % 2
    features, piece = points.shape

    def same_core(q):
        return (lax.rem(chip + q, chips) * 2 + core, w)

    sibling = (chip * 2 + 1 - core, w)

    def along(q):
        return (b, lax.rem(w + q, nw))

    def plane(slot):
        return (lax.rem(chip + slot // 2, chips) * 2 + (core if slot % 2 == 0 else 1 - core), w)

    def back(slot):
        return (chips - slot // 2) % chips * 2 + slot % 2

    barrier = pltpu.get_barrier_semaphore()
    for slot in range(1, nb):
        pl.semaphore_signal(barrier, inc=1, device_id=plane(slot), device_id_type=MESH)
    for q in range(1, nw):
        pl.semaphore_signal(barrier, inc=1, device_id=along(q), device_id_type=MESH)

    def copy(src, dst, send, recv, to):
        return pltpu.make_async_remote_copy(
            src_ref=src, dst_ref=dst, send_sem=send, recv_sem=recv, device_id=to, device_id_type=MESH
        )

    loads = [
        pltpu.make_async_copy(src, dst, io.at[k])
        for k, (src, dst) in enumerate(
            ((points_in, points), (inv_in, inv_length), (direction_in, direction),
             (residual_in, residual), (solution_in, old_solution))
        )
    ]
    for load in loads:
        load.start()
    for load in loads[:2]:
        load.wait()

    inv_row = jnp.concatenate(
        [inv_length[...], jnp.zeros((1, 128 - features), jnp.float32)], axis=1)
    inv_column = jnp.broadcast_to(inv_row, (8, 128)).T[:features, 0:1]
    x_t = rounded(points[...].astype(jnp.float32) * inv_column)
    s1, s2, s3 = three_parts(SCALE * jnp.sum(x_t * x_t, axis=0, keepdims=True))
    row = lax.broadcasted_iota(jnp.int32, (TAIL, piece), 0)
    tail = jnp.where((row >= 3) & (row <= 10), 1.0, 0.0)
    tail = jnp.where((row >= 6) & (row <= 7), 0.0, tail)
    for at, value in ((0, s1), (1, s2), (2, s3), (11, s1), (12, s2), (13, s3)):
        tail = jnp.where(row == at, value, tail)
    feat[0] = jnp.concatenate([x_t, tail], axis=0).astype(jnp.bfloat16)
    for load in loads[2:]:
        load.wait()
    low_dir[0:piece] = direction[...].astype(jnp.bfloat16)
    pl.semaphore_wait(barrier, nb - 1 + nw - 1)

    upper = lax.div(2 * w, nw)

    def near(k):
        return k + upper * (nw - 2 * k)

    def rows_at(q):
        return pl.ds(pl.multiple_of(q * piece, piece), piece)

    sends = []

    def go(c):
        c.start()
        sends.append(c)
        return c

    def feat_copy(src_slot, dst_slot, to):
        return copy(feat.at[src_slot], feat.at[dst_slot], fs.at[dst_slot], fr.at[dst_slot], to)

    def dir_copy(src_slot, dst_slot, to):
        return copy(low_dir.at[pl.ds(src_slot * piece, piece)], low_dir.at[pl.ds(dst_slot * piece, piece)],
                    ps.at[dst_slot], pr.at[dst_slot], to)

    for k in range(1, nw):
        q = near(nw - k)
        go(copy(feat.at[0], feat_z.at[nw - q], fzs.at[q], fzr.at[nw - q], along(q)))
    go(feat_copy(0, 1, sibling))
    for q in range(1, chips):
        go(feat_copy(0, 2 * (chips - q), same_core(q)))
    for q in range(1, chips):
        go(dir_copy(0, 2 * (chips - q), same_core(q)))
    go(dir_copy(0, 1, sibling))

    def feat_arrived(slot):
        feat_copy(slot, slot, sibling).wait_recv()

    def dir_arrived(slot):
        dir_copy(slot, slot, sibling).wait_recv()

    def as_rows(block):
        block = block.astype(jnp.float32)
        x = block[:features]
        h, m, l = three_parts(SCALE * x)
        lanes = jnp.concatenate(
            [-2.0 * h, -2.0 * m, -2.0 * l, block[features + 8 :],
             jnp.zeros((TAIL + 8, piece), jnp.float32)], axis=0)
        return lanes.T.astype(jnp.bfloat16)

    depth = rows_x.shape[1]

    def tile(at, slot):
        block = feat[slot]
        cols = jnp.concatenate(
            [block[:features]] * 3 + [block[features:],
             jnp.zeros((depth - 3 * features - TAIL, piece), jnp.bfloat16)], axis=0)
        dist = jnp.dot(rows_x[at, :], cols, preferred_element_type=jnp.float32)
        kmat[at, slot * piece : (slot + 1) * piece] = matern(dist)

    def feat_z_arrived(q):
        copy(feat_z.at[q], feat_z.at[q], fzs.at[q], fzr.at[q], along(q)).wait_recv()

    def relay_direction(q):
        dir_arrived(2 * q)
        go(dir_copy(2 * q, 2 * q + 1, sibling))

    rows_x[0:piece] = as_rows(feat[0])
    tile(pl.ds(0, piece), 0)
    feat_arrived(1)
    tile(pl.ds(0, piece), 1)
    for q in range(1, chips):
        feat_arrived(2 * q)
        go(feat_copy(2 * q, 2 * q + 1, sibling))
        tile(pl.ds(0, piece), 2 * q)
    for q in range(1, chips):
        feat_arrived(2 * q + 1)
        tile(pl.ds(0, piece), 2 * q + 1)
    if nw <= 4:
        relayed = 1
        for k in range(1, nw):
            q = near(k)
            feat_z_arrived(q)
            rows_x[rows_at(q), :] = as_rows(feat_z[q])
            for slot in range(nb):
                tile(rows_at(q), slot)
                if k == nw - 1 and slot in (0, nb // 2) and relayed < chips:
                    relay_direction(relayed)
                    relayed += 1
    else:
        relayed = 1
        for q in range(1, nw):
            feat_z_arrived(q)
            rows_x[q * piece : (q + 1) * piece] = as_rows(feat_z[q])

        def row_tiles(q, carry):
            for slot in range(nb):
                tile(pl.ds(pl.multiple_of(q * piece, piece), piece), slot)
            return carry

        lax.fori_loop(1, nw, row_tiles, 0)
    for q in range(relayed, chips):
        relay_direction(q)
    for q in range(chips):
        dir_arrived(2 * q + 1)

    def partial(q):
        return jnp.dot(kmat[rows_at(q), :], low_dir[...],
                       preferred_element_type=jnp.float32)

    for k in range(1, nw):
        q = near(nw - k)
        part[q] = partial(q).astype(jnp.bfloat16)
        go(copy(part.at[q], part_in.at[nw - q], qs.at[q], qr.at[nw - q], along(q)))
    total = partial(0) + noise_in[0, 0] * direction[...]
    for q in range(1, nw):
        copy(part.at[q], part_in.at[q], qs.at[q], qr.at[q], along(q)).wait_recv()
        total = total + part_in[q].astype(jnp.float32)

    def column_sum(x):
        return jnp.sum(x, axis=0, keepdims=True)

    res, direc = residual[...], direction[...]
    at = lax.broadcasted_iota(jnp.int32, (8, res.shape[1]), 0)
    sums = jnp.zeros(at.shape, jnp.float32)
    for k, value in enumerate((res * res, direc * total, res * total, total * total)):
        sums = jnp.where(at == k, column_sum(value), sums)
    stat[...] = sums
    for q in range(1, nw):
        go(copy(stat, stat_z.at[nw - q], zs.at[q], zr.at[nw - q], along(q)))
    for q in range(1, nw):
        copy(stat, stat_z.at[q], zs.at[q], zr.at[q], along(q)).wait_recv()
        sums = sums + stat_z[q]
    stat_o[...] = sums
    for slot in range(1, nb):
        go(copy(stat_o, stat_b.at[back(slot)], bs.at[slot], br.at[back(slot)], plane(slot)))
    for slot in range(1, nb):
        copy(stat_o, stat_b.at[slot], bs.at[slot], br.at[slot], plane(slot)).wait_recv()
        sums = sums + stat_b[slot]
    old_norm, step = sums[0:1], sums[0:1] / sums[1:2]
    new_norm = old_norm - 2.0 * step * sums[2:3] + step * step * sums[3:4]
    new_residual = res - step * total
    residual_out[...] = new_residual
    solution_out[...] = old_solution[...] + step * direc
    direction_out[...] = new_residual + new_norm / old_norm * direc
    for c in sends:
        c.wait_send()


def write_out(a, b, c, a_out, b_out, c_out, sems):
    copies = [
        pltpu.make_async_copy(src, dst, sems.at[k])
        for k, (src, dst) in enumerate(((a, a_out), (b, b_out), (c, c_out)))
    ]
    for copy in copies:
        copy.start()
    for copy in copies:
        copy.wait()


def on_device(nb, nw, points, inv_length, noise_var, solution, residual, direction):
    piece, features = points.shape
    rhs = direction.shape[1]
    vmem = pl.BlockSpec(memory_space=pltpu.VMEM)
    hbm = pl.BlockSpec(memory_space=pl.ANY)
    dma = pltpu.SemaphoreType.DMA
    depth = 3 * features + 2 * TAIL
    common = [
        pltpu.VMEM((features, piece), points.dtype),
        pltpu.VMEM((1, features), jnp.float32),
    ]
    wide = [
        dma((6,)),
        pltpu.VMEM((nb, features + TAIL, piece), jnp.bfloat16),
        pltpu.VMEM((nw, features + TAIL, piece), jnp.bfloat16),
        pltpu.VMEM((nw * piece, depth), jnp.bfloat16),
        pltpu.VMEM((nw * piece, nb * piece), jnp.bfloat16),
        pltpu.VMEM((nb * piece, rhs), jnp.bfloat16),
    ]
    vectors = [pltpu.VMEM((piece, rhs), jnp.float32)] * 3
    parts = [pltpu.VMEM((nw, piece, rhs), jnp.bfloat16)] * 2
    sems = [dma((nb,)), dma((nb,)), dma((nw,)), dma((nw,)), dma((nb,)), dma((nb,)), dma((nw,)), dma((nw,))]
    if nw <= 4:
        body = kernel
        half = rhs // 2
        low = jnp.bfloat16
        scratch = common + [
            pltpu.VMEM((piece, rhs), jnp.float32), pltpu.VMEM((2, piece, rhs), jnp.float32), dma((4,)),
            pltpu.VMEM((nb, features, piece), low), pltpu.VMEM((nw, features, piece), low),
            pltpu.VMEM((nw * piece, depth), low), pltpu.VMEM((nb, depth, piece), low),
            pltpu.VMEM((nw * piece, nb * piece), low),
            pltpu.VMEM((nb, half, piece), low), pltpu.VMEM((nw, half, piece), low),
            pltpu.VMEM((nb * piece, half), low),
            pltpu.VMEM((nw, half, piece), low), pltpu.VMEM((nw, half, piece), low),
            pltpu.VMEM((nb, half, piece), low), pltpu.VMEM((nb, half, piece), low),
            pltpu.VMEM((4, rhs), jnp.float32), pltpu.VMEM((nw * nb, 4, rhs), jnp.float32),
            dma((7,)), dma((nb - 1,)), dma((nw - 1,)), dma((nb // 2,)), dma((4,)),
        ]
    else:
        body = long_kernel
        scratch = common + [pltpu.VMEM((1, 1), jnp.float32)] + vectors + wide + parts + [
            pltpu.VMEM((8, rhs), jnp.float32),
            pltpu.VMEM((nw, 8, rhs), jnp.float32),
            pltpu.VMEM((nb, 8, rhs), jnp.float32),
            pltpu.VMEM((8, rhs), jnp.float32),
        ] + sems + [dma((nw,)), dma((nw,)), dma((nb,)), dma((nb,))]
    news = pl.pallas_call(
        functools.partial(body, nb, nw),
        out_shape=(pltpu.VMEM((piece, rhs), jnp.float32),) * 3,
        in_specs=[hbm, hbm, pl.BlockSpec(memory_space=pltpu.SMEM), hbm, hbm, hbm],
        out_specs=(vmem,) * 3,
        scratch_shapes=scratch,
        compiler_params=pltpu.CompilerParams(
            collective_id=0, has_side_effects=True, vmem_limit_bytes=60 * 1024 * 1024
        ),
    )(points.T, inv_length.reshape(1, features), noise_var.reshape(1, 1), residual, direction, solution)
    return pl.pallas_call(
        write_out,
        out_shape=(jax.ShapeDtypeStruct((piece, rhs), jnp.float32),) * 3,
        in_specs=[vmem] * 3,
        out_specs=(hbm,) * 3,
        scratch_shapes=[dma((3,))],
    )(*(pltpu.with_memory_space_constraint(x, pltpu.VMEM) for x in news))


def solution(mesh):
    spec = P(("blk", "wide"), None)
    return jax.shard_map(
        functools.partial(on_device, mesh.shape["blk"], mesh.shape["wide"]),
        mesh=mesh,
        in_specs=(spec, P(), P(), spec, spec, spec),
        out_specs=(spec, spec, spec),
        check_vma=False,
    )
```
